32 devices in a mesh: att: 8 (over z, y), emb: 4 (over x, core).
Axes of the slice: x: 2, y: 2, z: 4, core: 2. Of those that a mesh axis runs over, the one named last changes fastest.
Arguments:
- w_qkv: float32 [4, 3, 2048, 2048], P(None, None, 'emb', 'att')
- w_out: float32 [4, 2048, 2048], P(None, 'att', 'emb')
- x_in: bfloat16 [4, 6144, 2048], P(None, None, 'emb')
- dy_qkv: bfloat16 [4, 3, 6144, 2048], P(None, None, None, 'att')
- x_attn: bfloat16 [4, 6144, 2048], P(None, None, 'att')
- dy_out: bfloat16 [4, 6144, 2048], P(None, None, 'emb')
- r_qkv: float32 [4, 3, 2048], P(None, None, 'emb')
- c_qkv: float32 [4, 3, 2048], P(None, None, 'att')
- r_out: float32 [4, 2048], P(None, 'att')
- c_out: float32 [4, 2048], P(None, 'emb')
- hyper_params: float32 [3], replicated
Outputs:
- output 1: float32 [4, 3, 2048, 2048], P(None, None, 'emb', 'att')
- output 2: float32 [4, 2048, 2048], P(None, 'att', 'emb')
- output 3: float32 [4, 3, 2048], P(None, None, 'emb')
- output 4: float32 [4, 3, 2048], P(None, None, 'att')
- output 5: float32 [4, 2048], P(None, 'att')
- output 6: float32 [4, 2048], P(None, 'emb')
All inputs are finite; a program needn't handle non-finite values.
Results may differ from the reference program's by a relative error of at most 0.001.
Values are sent between devices in bfloat16 or wider.
A program may use at most 1 GiB of HBM per device.

```python
import functools
import jax
import jax.numpy as jnp
from jax import lax

D = 2048
HEADS = 32
HEAD = 64
TOKENS = 6144
LAYERS = 4

INNER = HEADS * HEAD
EPS_SQUARE = 1e-30
EPS_SCALE = 1e-3


def cos_scale(rng_key, lead_shape, length, amplitude):
    phase_off = jax.random.uniform(rng_key, lead_shape + (1,), jnp.float32)
    position = jnp.arange(length, dtype=jnp.float32) / length
    return jnp.exp(amplitude * jnp.cos(2.0 * jnp.pi * (position + phase_off)))


def scaled_tokens(rng_key, lead_shape, length, factor):
    key_noise, key_scale = jax.random.split(rng_key)
    gauss_noise = jax.random.normal(key_noise, lead_shape + (2, TOKENS // 2, length), jnp.float32)
    scales = cos_scale(key_scale, lead_shape + (2, 1), length, 0.75)
    return (gauss_noise * scales * factor).reshape(lead_shape + (TOKENS, length)).astype(jnp.bfloat16)


def scaled_weight(rng_key, lead_shape, n_rows, n_cols):
    key_noise, key_row, key_col = jax.random.split(rng_key, 3)
    gauss_noise = jax.random.normal(key_noise, lead_shape + (n_rows, n_cols), jnp.float32)
    row_scale = cos_scale(key_row, lead_shape, n_rows, 0.5)
    col_scale = cos_scale(key_col, lead_shape, n_cols, 0.5)
    return gauss_noise * row_scale[..., :, None] * col_scale[..., None, :] * n_rows ** -0.5


def setup_inputs(seed: int = 0) -> dict:
    key_list = jax.random.split(jax.random.key(seed), 11)
    tok_norm = TOKENS ** -0.5
    low_end = jnp.array([0.5, 0.5, 0.2], jnp.float32)
    high_end = jnp.array([0.8, 1.0, 0.4], jnp.float32)
    return {
        "w_qkv": scaled_weight(key_list[0], (LAYERS, 3), D, INNER),
        "w_out": scaled_weight(key_list[1], (LAYERS,), INNER, D),
        "x_in": scaled_tokens(key_list[2], (LAYERS,), D, 1.0),
        "dy_qkv": scaled_tokens(key_list[3], (LAYERS, 3), INNER, tok_norm),
        "x_attn": scaled_tokens(key_list[4], (LAYERS,), INNER, 1.0),
        "dy_out": scaled_tokens(key_list[5], (LAYERS,), D, tok_norm),
        "r_qkv": jax.random.uniform(key_list[6], (LAYERS, 3, D), jnp.float32, 0.2, 1.0),
        "c_qkv": jax.random.uniform(key_list[7], (LAYERS, 3, INNER), jnp.float32, 0.2, 1.0),
        "r_out": jax.random.uniform(key_list[8], (LAYERS, INNER), jnp.float32, 0.2, 1.0),
        "c_out": jax.random.uniform(key_list[9], (LAYERS, D), jnp.float32, 0.2, 1.0),
        "hyper_params": jax.random.uniform(key_list[10], (3,), jnp.float32, low_end, high_end),
    }


def adafactor_one(w_grad, weight, row_old, col_old, hyper_params):
    beta_two = hyper_params[0]
    rel_step = hyper_params[1]
    clip_limit = hyper_params[2]
    q_sq = w_grad * w_grad + EPS_SQUARE
    row_new = beta_two * row_old + (1.0 - beta_two) * jnp.mean(q_sq, axis=1)
    col_new = beta_two * col_old + (1.0 - beta_two) * jnp.mean(q_sq, axis=0)
    second = row_new[:, None] * col_new[None, :] / jnp.mean(row_new)
    update = w_grad / jnp.sqrt(second)
    rms_u = jnp.sqrt(jnp.mean(update * update))
    clipped = update / jnp.maximum(1.0, rms_u / clip_limit)
    step_size = rel_step * jnp.maximum(EPS_SCALE, jnp.sqrt(jnp.mean(weight * weight)))
    return weight - step_size * clipped, row_new, col_new


def reference(w_qkv, w_out, x_in, dy_qkv, x_attn, dy_out, r_qkv, c_qkv, r_out, c_out, hyper_params):
    step_fn = functools.partial(adafactor_one, hyper_params=hyper_params)

    def one_layer(carry, layer_in):
        lw_qkv, lw_out, lx_in, ldy_qkv, lx_attn, ldy_out, lr_qkv, lc_qkv, lr_out, lc_out = layer_in
        g_qkv = jnp.einsum("td,ktn->kdn", lx_in.astype(jnp.float32), ldy_qkv.astype(jnp.float32))
        g_out = jnp.dot(lx_attn.T, ldy_out, preferred_element_type=jnp.float32)
        new_qkv = jax.vmap(step_fn)(g_qkv, lw_qkv, lr_qkv, lc_qkv)
        new_out = step_fn(g_out, lw_out, lr_out, lc_out)
        return carry, (new_qkv[0], new_out[0], new_qkv[1], new_qkv[2], new_out[1], new_out[2])

    final_carry, results = lax.scan(
        one_layer,
        jnp.zeros((), jnp.float32),
        (w_qkv, w_out, x_in, dy_qkv, x_attn, dy_out, r_qkv, c_qkv, r_out, c_out),
    )
    return (results[0], results[1], results[2], results[3], results[4], results[5])
```

```python
import functools

import jax
import jax.numpy as jnp
from jax import lax
from jax.experimental import pallas as pl
from jax.experimental.pallas import tpu as pltpu
from jax.sharding import PartitionSpec as P

EPS_SQUARE = 1e-30
EPS_SCALE = 1e-3
F32 = jnp.float32
BF16 = jnp.bfloat16
MESH = pl.DeviceIdType.MESH
TB = 1024
NA = 6
NB = 6
ATT = 8
EMB = 4


def rows_to_lanes(part):
    return jnp.sum(part.T, axis=0, keepdims=True)


def fold8(part):
    return jnp.sum(part.reshape(part.shape[0] // 8, 8, 128), axis=0)


def total(part):
    return jnp.sum(jnp.sum(part, axis=0, keepdims=True), axis=1, keepdims=True)


def step_kernel(
    n_layers, n_tokens, d_model,
    hyper, x_in, dy_qkv, x_attn, dy_out, w_qkv, w_out, r_qkv, c_qkv, r_out, c_out,
    u_qkv, u_out, wv_qkv, wv_out, scales, rn_qkv, cn_qkv, rn_out, cn_out,
    xb, dyb, xab, dob, rq, cq, ro, co, row_a, row_b,
    att_a, emb_a, att_b, emb_b, glob, old_a, old_ac, old_b, old_bc, payload,
    sem_a, sem_b, sem_w, sem_s, send_sem, recv_sem, send_g, recv_g,
):
    nb = n_tokens // TB
    me_att = lax.axis_index("att")
    me_emb = lax.axis_index("emb")

    def copies_a(g):
        l, i, s = g // nb, g % nb, g % NA
        t = pl.ds(pl.multiple_of(i * TB, TB), TB)
        return (
            pltpu.make_async_copy(x_in.at[l, t], xb.at[s], sem_a.at[s, 0]),
            pltpu.make_async_copy(dy_qkv.at[l, :, t], dyb.at[s], sem_a.at[s, 1]),
        )

    def copies_b(g):
        l, i, s = g // nb, g % nb, g % NB
        t = pl.ds(pl.multiple_of(i * TB, TB), TB)
        return (
            pltpu.make_async_copy(x_attn.at[l, t], xab.at[s], sem_b.at[s, 0]),
            pltpu.make_async_copy(dy_out.at[l, t], dob.at[s], sem_b.at[s, 1]),
        )

    def copies_w(l):
        return (
            pltpu.make_async_copy(w_qkv.at[l], wv_qkv.at[l], sem_w.at[l, 0]),
            pltpu.make_async_copy(w_out.at[l], wv_out.at[l], sem_w.at[l, 1]),
        )

    def start(copies):
        for copy in copies:
            copy.start()

    def wait(copies):
        for copy in copies:
            copy.wait()

    def send_att(buf, kind, l):
        for d in (4, 3, 5, 2, 6, 1, 7):
            pltpu.make_async_remote_copy(
                src_ref=buf.at[l, 0], dst_ref=buf.at[l, ATT - d],
                send_sem=send_sem.at[kind, l], recv_sem=recv_sem.at[kind, l],
                device_id={"att": lax.rem(me_att + d, ATT)}, device_id_type=MESH,
            ).start()

    def send_emb(buf, kind, l):
        for d in (2, 1, 3):
            pltpu.make_async_remote_copy(
                src_ref=buf.at[l, 0], dst_ref=buf.at[l, EMB - d],
                send_sem=send_sem.at[kind, l], recv_sem=recv_sem.at[kind, l],
                device_id={"emb": lax.rem(me_emb + d, EMB)}, device_id_type=MESH,
            ).start()

    def wait_group(buf, n, kind, l):
        others = buf.at[l, pl.ds(1, n - 1)]
        pltpu.make_async_copy(others, others, send_sem.at[kind, l]).wait()
        pltpu.make_async_copy(others, others, recv_sem.at[kind, l]).wait()

    for g in range(NA):
        start(copies_a(jnp.int32(g)))
        start(copies_b(jnp.int32(g)))
    small = [
        pltpu.make_async_copy(src, dst, sem_s.at[n])
        for n, (src, dst) in enumerate(((r_qkv, rq), (c_qkv, cq), (r_out, ro), (c_out, co)))
    ]
    start(small)

    barrier = pltpu.get_barrier_semaphore()
    for da in range(ATT):
        for de in range(EMB):
            if da or de:
                pl.semaphore_signal(
                    barrier, inc=1,
                    device_id={"att": lax.rem(me_att + da, ATT), "emb": lax.rem(me_emb + de, EMB)},
                    device_id_type=MESH,
                )
    payload[...] = jnp.zeros_like(payload)
    wait(small)
    for l in range(n_layers):
        for k in range(3):
            for j in range(4):
                old_a[l, k * 4 + j : k * 4 + j + 1, :] = rq[k, l : l + 1, j * 128 : (j + 1) * 128]
            for j in range(2):
                old_ac[l, k * 2 + j : k * 2 + j + 1, :] = cq[k, l : l + 1, j * 128 : (j + 1) * 128]
        for j in range(2):
            old_b[l, j : j + 1, :] = ro[l : l + 1, j * 128 : (j + 1) * 128]
        for j in range(4):
            old_bc[l, j : j + 1, :] = co[l : l + 1, j * 128 : (j + 1) * 128]
    pl.semaphore_wait(barrier, ATT * EMB - 1)

    beta = hyper[0]
    gain = 1.0 - beta

    def zero(l):
        u_qkv[l] = jnp.zeros_like(u_qkv[l])
        u_out[l] = jnp.zeros_like(u_out[l])

    def mul_a(l, s):
        grads = jnp.concatenate([dyb[s, k] for k in range(3)], axis=1)
        prod = lax.dot_general(xb[s], grads, (((0,), (0,)), ((), ())), preferred_element_type=F32)
        for k in range(3):
            u_qkv[l, k] = u_qkv[l, k] + prod[:, k * 256 : (k + 1) * 256]

    def mul_b(l, s):
        prod = lax.dot_general(xab[s], dob[s], (((0,), (0,)), ((), ())), preferred_element_type=F32)
        u_out[l] = u_out[l] + prod

    def refill_a(g):
        @pl.when(g + NA < n_layers * nb)
        def _():
            start(copies_a(g + NA))

    def refill_b(g):
        @pl.when(g + NB < n_layers * nb)
        def _():
            start(copies_b(g + NB))

    def stats_a(l):
        for k in range(3):
            cols = None
            for q in range(2):
                g = u_qkv[l, k, pl.ds(q * 256, 256)]
                sq = g * g
                row_a[k, pl.ds(q * 256, 256)] = sq[:, :128] + sq[:, 128:]
                part = jnp.sum(sq, axis=0, keepdims=True)
                cols = part if cols is None else cols + part
            for j in range(2):
                emb_a[l, 0, k * 2 + j : k * 2 + j + 1, :] = cols[:, j * 128 : (j + 1) * 128]
        for k in range(3):
            rows = rows_to_lanes(row_a[k])
            for j in range(4):
                att_a[l, 0, k * 4 + j : k * 4 + j + 1, :] = rows[:, j * 128 : (j + 1) * 128]
        send_att(att_a, 0, l)
        send_emb(emb_a, 1, l)

    def stats_b(l):
        parts = []
        for q in range(2):
            g = u_out[l, :, pl.ds(q * 256, 256)]
            sq = g * g
            parts.append(sq[:, :128] + sq[:, 128:])
            cols = jnp.sum(sq, axis=0, keepdims=True)
            for j in range(2):
                att_b[l, 0, q * 2 + j : q * 2 + j + 1, :] = cols[:, j * 128 : (j + 1) * 128]
            if q == 0:
                row_b[...] = parts[0]
            else:
                row_b[...] = row_b[...] + parts[1]
        rows = rows_to_lanes(row_b[...])
        for j in range(2):
            emb_b[l, 0, j : j + 1, :] = rows[:, j * 128 : (j + 1) * 128]
        send_att(att_b, 2, l)
        send_emb(emb_b, 3, l)

    def record(slot, value):
        lane = lax.broadcasted_iota(jnp.int32, (1, 128), 1)
        payload[...] = jnp.where(lane == slot, value, payload[...])

    def sum_w(l):
        wait(copies_w(l))
        for k in range(3):
            w = wv_qkv[l, k]
            record(32 + l * 4 + k, total(fold8(w[:, :128] * w[:, :128] + w[:, 128:] * w[:, 128:])))
        w = wv_out[l]
        part = sum(fold8(w[:, j * 128 : (j + 1) * 128] * w[:, j * 128 : (j + 1) * 128]) for j in range(4))
        record(32 + l * 4 + 3, total(part))

    def apply_a(l):
        wait_group(att_a, ATT, 0, l)
        wait_group(emb_a, EMB, 1, l)
        row_sum = att_a[l, 0]
        for d in range(1, ATT):
            row_sum = row_sum + att_a[l, d]
        col_sum = emb_a[l, 0]
        for d in range(1, EMB):
            col_sum = col_sum + emb_a[l, d]
        r_new = beta * old_a[l] + gain * (row_sum * (1.0 / d_model) + EPS_SQUARE)
        c_new = beta * old_ac[l] + gain * (col_sum * (1.0 / d_model) + EPS_SQUARE)
        rn_qkv[l] = r_new
        cn_qkv[l] = c_new
        b_all = lax.rsqrt(c_new)
        for k in range(3):
            r_k = r_new[k * 4 : (k + 1) * 4]
            mean = total(r_k) * (1.0 / 512)
            a_k = lax.rsqrt(r_k / mean)
            tsum = jnp.zeros((8, 128), F32)
            for j in range(4):
                a_col = jnp.broadcast_to(a_k[j : j + 1], (128, 128)).T
                for h in range(2):
                    rr, cc = pl.ds(j * 128, 128), pl.ds(h * 128, 128)
                    u = u_qkv[l, k, rr, cc] * a_col * b_all[k * 2 + h : k * 2 + h + 1]
                    u_qkv[l, k, rr, cc] = u
                    tsum = tsum + fold8(u * u)
            record(l * 4 + k, total(tsum))
            record(16 + l * 4 + k, mean)

    def apply_b(l):
        wait_group(att_b, ATT, 2, l)
        wait_group(emb_b, EMB, 3, l)
        col_sum = att_b[l, 0]
        for d in range(1, ATT):
            col_sum = col_sum + att_b[l, d]
        row_sum = emb_b[l, 0]
        for d in range(1, EMB):
            row_sum = row_sum + emb_b[l, d]
        r_new = beta * old_b[l] + gain * (row_sum * (1.0 / d_model) + EPS_SQUARE)
        c_new = beta * old_bc[l] + gain * (col_sum * (1.0 / d_model) + EPS_SQUARE)
        b_all = lax.rsqrt(c_new)
        mean = total(r_new) * (1.0 / 256)
        a_all = lax.rsqrt(r_new / mean)
        tsum = jnp.zeros((8, 128), F32)
        for j in range(2):
            a_col = jnp.broadcast_to(a_all[j : j + 1], (128, 128)).T
            for h in range(4):
                rr, cc = pl.ds(j * 128, 128), pl.ds(h * 128, 128)
                u = u_out[l, rr, cc] * a_col * b_all[h : h + 1]
                u_out[l, rr, cc] = u
                tsum = tsum + fold8(u * u)
        rn_out[l] = r_new
        cn_out[l] = c_new
        record(l * 4 + 3, total(tsum))
        record(16 + l * 4 + 3, mean)

    last = n_layers - 1

    def layer(l, carry):
        start(copies_w(l))
        zero(l)

        def block(i, carry):
            g = l * nb + i
            wait(copies_a(g))
            wait(copies_b(g))
            mul_a(l, g % NA)
            mul_b(l, g % NB)
            refill_a(g)
            refill_b(g)

            @pl.when((i == 3) & (l > 0))
            def _():
                sum_w(l - 1)
                apply_a(l - 1)
                apply_b(l - 1)

            return carry

        lax.fori_loop(0, nb, block, 0)
        stats_a(l)
        stats_b(l)
        return carry

    lax.fori_loop(0, last, layer, 0)
    start(copies_w(last))
    zero(last)

    def block_a(i, carry):
        g = last * nb + i
        wait(copies_a(g))
        mul_a(last, g % NA)

        @pl.when(i == 3)
        def _():
            sum_w(last - 1)
            apply_a(last - 1)
            apply_b(last - 1)

        return carry

    lax.fori_loop(0, nb, block_a, 0)
    stats_a(last)

    def block_b(i, carry):
        g = last * nb + i
        wait(copies_b(g))
        mul_b(last, g % NB)
        return carry

    lax.fori_loop(0, nb, block_b, 0)
    stats_b(last)
    sum_w(last)
    apply_a(last)
    apply_b(last)

    glob[0] = payload[...]
    for da in (4, 3, 5, 2, 6, 1, 7, 0):
        for de in (2, 3, 1, 0):
            if da or de:
                pltpu.make_async_remote_copy(
                    src_ref=glob.at[0], dst_ref=glob.at[((ATT - da) % ATT) * EMB + (EMB - de) % EMB],
                    send_sem=send_g, recv_sem=recv_g,
                    device_id={"att": lax.rem(me_att + da, ATT), "emb": lax.rem(me_emb + de, EMB)},
                    device_id_type=MESH,
                ).start()
    others = glob.at[pl.ds(1, ATT * EMB - 1)]
    pltpu.make_async_copy(others, others, send_g).wait()
    pltpu.make_async_copy(others, others, recv_g).wait()
    n_dev = ATT * EMB
    mean_sum = jnp.zeros((1, 128), F32)
    w_sum = jnp.zeros((1, 128), F32)
    u_sum = jnp.zeros((1, 128), F32)
    for d in range(n_dev):
        row = glob[d]
        local_mean = pltpu.roll(row, 128 - 16, 1)
        mean_sum = mean_sum + local_mean
        w_sum = w_sum + pltpu.roll(row, 128 - 32, 1)
    mean_all = mean_sum * (1.0 / n_dev)
    for d in range(n_dev):
        row = glob[d]
        u_sum = u_sum + row * (mean_all / pltpu.roll(row, 128 - 16, 1))
    n_elems = float(d_model) * d_model
    rms_u = jnp.sqrt(u_sum * (1.0 / n_elems))
    rms_w = jnp.sqrt(w_sum * (1.0 / n_elems))
    step = hyper[1] * jnp.maximum(EPS_SCALE, rms_w) / jnp.maximum(1.0, rms_u / hyper[2])
    scales[...] = step * jnp.sqrt(mean_all / pltpu.roll(payload[...], 128 - 16, 1))


def write_kernel(
    n_layers, u_qkv, u_out, wv_qkv, wv_out, scales, rn_qkv, cn_qkv, rn_out, cn_out,
    wn_qkv, wn_out, r_qkv, c_qkv, r_out, c_out,
    st_a, st_b, st_rq, st_cq, st_r, st_c, sem_w, sem_s,
):
    for l in range(n_layers):
        for k in range(3):
            for j in range(4):
                st_rq[k, l : l + 1, j * 128 : (j + 1) * 128] = rn_qkv[l, k * 4 + j : k * 4 + j + 1]
            for j in range(2):
                st_cq[k, l : l + 1, j * 128 : (j + 1) * 128] = cn_qkv[l, k * 2 + j : k * 2 + j + 1]
        for j in range(2):
            st_r[l : l + 1, j * 128 : (j + 1) * 128] = rn_out[l, j : j + 1]
        for j in range(4):
            st_c[l : l + 1, j * 128 : (j + 1) * 128] = cn_out[l, j : j + 1]
    small = [
        pltpu.make_async_copy(src, dst, sem_s.at[n])
        for n, (src, dst) in enumerate(((st_rq, r_qkv), (st_cq, c_qkv), (st_r, r_out), (st_c, c_out)))
    ]
    for copy in small:
        copy.start()
    copies = []
    for l in range(n_layers):
        for k in range(4):
            m = l * 4 + k
            s = scales[0:1, m : m + 1]
            if k < 3:
                st_a[l, k] = wv_qkv[l, k] - s * u_qkv[l, k]
                copy = pltpu.make_async_copy(st_a.at[l, k], wn_qkv.at[l, k], sem_w.at[m])
            else:
                st_b[l] = wv_out[l] - s * u_out[l]
                copy = pltpu.make_async_copy(st_b.at[l], wn_out.at[l], sem_w.at[m])
            copy.start()
            copies.append(copy)
    for copy in copies + small:
        copy.wait()


def solution(mesh):
    att, emb = mesh.shape["att"], mesh.shape["emb"]
    qkv = P(None, None, "emb", "att")
    out = P(None, "att", "emb")
    row = P(None, None, "emb")
    col = P(None, None, "att")

    def local_run(w_qkv, w_out, x_in, dy_qkv, x_attn, dy_out, r_qkv, c_qkv, r_out, c_out, hyper_params):
        n_layers, n_tokens = x_in.shape[:2]
        d_model = x_in.shape[2] * emb
        hbm = pl.BlockSpec(memory_space=pltpu.HBM)
        vmem = pl.BlockSpec(memory_space=pltpu.VMEM)
        smem = pl.BlockSpec(memory_space=pltpu.SMEM)
        like = lambda x: jax.ShapeDtypeStruct(x.shape, x.dtype)
        kept = lambda x: pltpu.VMEM(x.shape, x.dtype)
        stat = lambda n: pltpu.VMEM((n_layers, n, 128), F32)
        r_qkv, c_qkv = jnp.swapaxes(r_qkv, 0, 1), jnp.swapaxes(c_qkv, 0, 1)
        mids = pl.pallas_call(
            functools.partial(step_kernel, n_layers, n_tokens, d_model),
            out_shape=(
                kept(w_qkv), kept(w_out), kept(w_qkv), kept(w_out), pltpu.VMEM((1, 128), F32),
                stat(12), stat(6), stat(2), stat(4),
            ),
            in_specs=[smem] + [hbm] * 10,
            out_specs=[vmem] * 9,
            scratch_shapes=[
                pltpu.VMEM((NA, TB, 512), BF16), pltpu.VMEM((NA, 3, TB, 256), BF16),
                pltpu.VMEM((NB, TB, 256), BF16), pltpu.VMEM((NB, TB, 512), BF16),
                pltpu.VMEM(r_qkv.shape, F32), pltpu.VMEM(c_qkv.shape, F32),
                pltpu.VMEM(r_out.shape, F32), pltpu.VMEM(c_out.shape, F32),
                pltpu.VMEM((3, 512, 128), F32), pltpu.VMEM((256, 128), F32),
                pltpu.VMEM((n_layers, ATT, 12, 128), F32), pltpu.VMEM((n_layers, EMB, 6, 128), F32),
                pltpu.VMEM((n_layers, ATT, 4, 128), F32), pltpu.VMEM((n_layers, EMB, 2, 128), F32),
                pltpu.VMEM((ATT * EMB, 1, 128), F32),
                pltpu.VMEM((n_layers, 12, 128), F32), pltpu.VMEM((n_layers, 6, 128), F32),
                pltpu.VMEM((n_layers, 2, 128), F32), pltpu.VMEM((n_layers, 4, 128), F32),
                pltpu.VMEM((1, 128), F32),
                pltpu.SemaphoreType.DMA((NA, 2)), pltpu.SemaphoreType.DMA((NB, 2)),
                pltpu.SemaphoreType.DMA((n_layers, 2)), pltpu.SemaphoreType.DMA((4,)),
                pltpu.SemaphoreType.DMA((4, n_layers)), pltpu.SemaphoreType.DMA((4, n_layers)),
                pltpu.SemaphoreType.DMA, pltpu.SemaphoreType.DMA,
            ],
            compiler_params=pltpu.CompilerParams(
                collective_id=0, has_side_effects=True, vmem_limit_bytes=45 * 2**20
            ),
            name="adafactor_step",
        )(hyper_params, x_in, dy_qkv, x_attn, dy_out, w_qkv, w_out, r_qkv, c_qkv, r_out, c_out)
        wn_qkv, wn_out, rn_qkv, cn_qkv, rn_out, cn_out = pl.pallas_call(
            functools.partial(write_kernel, n_layers),
            out_shape=(like(w_qkv), like(w_out), like(r_qkv), like(c_qkv), like(r_out), like(c_out)),
            in_specs=[vmem] * 9,
            out_specs=[hbm] * 6,
            scratch_shapes=[
                pltpu.VMEM(w_qkv.shape, F32), pltpu.VMEM(w_out.shape, F32),
                pltpu.VMEM(r_qkv.shape, F32), pltpu.VMEM(c_qkv.shape, F32),
                pltpu.VMEM(r_out.shape, F32), pltpu.VMEM(c_out.shape, F32),
                pltpu.SemaphoreType.DMA((4 * n_layers,)), pltpu.SemaphoreType.DMA((4,)),
            ],
            compiler_params=pltpu.CompilerParams(vmem_limit_bytes=16 * 2**20),
            name="adafactor_write",
        )(*mids)
        return wn_qkv, wn_out, jnp.swapaxes(rn_qkv, 0, 1), jnp.swapaxes(cn_qkv, 0, 1), rn_out, cn_out

    return jax.shard_map(
        local_run,
        mesh=mesh,
        in_specs=(qkv, out, row, P(None, None, None, "att"), col, row, row, col, P(None, "att"), P(None, "emb"), P()),
        out_specs=(qkv, out, row, col, P(None, "att"), P(None, "emb")),
        check_vma=False,
    )
```

```python
import functools

import jax
import jax.numpy as jnp
from jax import lax
from jax.experimental import pallas as pl
from jax.experimental.pallas import tpu as pltpu
from jax.sharding import PartitionSpec as P

EPS_SQUARE = 1e-30
EPS_SCALE = 1e-3
F32 = jnp.float32
BF16 = jnp.bfloat16
MESH = pl.DeviceIdType.MESH
TB = 2048
NA = 3
NB = 3
ATT = 8
EMB = 4


def rows_to_lanes(part):
    return jnp.sum(part.T, axis=0, keepdims=True)


def fold8(part):
    return jnp.sum(part.reshape(part.shape[0] // 8, 8, 128), axis=0)


def total(part):
    return jnp.sum(jnp.sum(part, axis=0, keepdims=True), axis=1, keepdims=True)


def step_kernel(
    n_layers, n_tokens, d_model,
    hyper, x_in, dy_qkv, x_attn, dy_out, w_qkv, w_out, r_qkv, c_qkv, r_out, c_out,
    u_qkv, u_out, wv_qkv, wv_out, scales, rn_qkv, cn_qkv, rn_out, cn_out,
    xb, dyb, xab, dob, rq, cq, ro, co, row_a, row_b,
    att_a, emb_a, att_b, emb_b, glob, old_a, old_ac, old_b, old_bc, payload,
    sem_a, sem_b, sem_w, sem_s, send_sem, recv_sem, send_g, recv_g,
):
    nb = n_tokens // TB
    me_att = lax.axis_index("att")
    me_emb = lax.axis_index("emb")

    def copies_a(g):
        l, i, s = g // nb, g % nb, g % NA
        t = pl.ds(pl.multiple_of(i * TB, TB), TB)
        return (
            pltpu.make_async_copy(x_in.at[l, t], xb.at[s], sem_a.at[s, 0]),
            pltpu.make_async_copy(dy_qkv.at[l, :, t], dyb.at[s], sem_a.at[s, 1]),
        )

    def copies_b(g):
        l, i, s = g // nb, g % nb, g % NB
        t = pl.ds(pl.multiple_of(i * TB, TB), TB)
        return (
            pltpu.make_async_copy(x_attn.at[l, t], xab.at[s], sem_b.at[s, 0]),
            pltpu.make_async_copy(dy_out.at[l, t], dob.at[s], sem_b.at[s, 1]),
        )

    def copies_w(l):
        return (
            pltpu.make_async_copy(w_qkv.at[l], wv_qkv.at[l], sem_w.at[l, 0]),
            pltpu.make_async_copy(w_out.at[l], wv_out.at[l], sem_w.at[l, 1]),
        )

    def start(copies):
        for copy in copies:
            copy.start()

    def wait(copies):
        for copy in copies:
            copy.wait()

    def send_att(buf, kind, l):
        for d in (4, 3, 5, 2, 6, 1, 7):
            pltpu.make_async_remote_copy(
                src_ref=buf.at[l, 0], dst_ref=buf.at[l, ATT - d],
                send_sem=send_sem.at[kind, l], recv_sem=recv_sem.at[kind, l],
                device_id={"att": lax.rem(me_att + d, ATT)}, device_id_type=MESH,
            ).start()

    def send_emb(buf, kind, l):
        for d in (2, 1, 3):
            pltpu.make_async_remote_copy(
                src_ref=buf.at[l, 0], dst_ref=buf.at[l, EMB - d],
                send_sem=send_sem.at[kind, l], recv_sem=recv_sem.at[kind, l],
                device_id={"emb": lax.rem(me_emb + d, EMB)}, device_id_type=MESH,
            ).start()

    def wait_group(buf, n, kind, l):
        others = buf.at[l, pl.ds(1, n - 1)]
        pltpu.make_async_copy(others, others, send_sem.at[kind, l]).wait()
        pltpu.make_async_copy(others, others, recv_sem.at[kind, l]).wait()

    small = [
        pltpu.make_async_copy(src, dst, sem_s.at[n])
        for n, (src, dst) in enumerate(((r_qkv, rq), (c_qkv, cq), (r_out, ro), (c_out, co)))
    ]
    start(small)
    for g in range(NA):
        start(copies_a(jnp.int32(g)))
        start(copies_b(jnp.int32(g)))

    barrier = pltpu.get_barrier_semaphore()
    for da in range(ATT):
        for de in range(EMB):
            if da or de:
                pl.semaphore_signal(
                    barrier, inc=1,
                    device_id={"att": lax.rem(me_att + da, ATT), "emb": lax.rem(me_emb + de, EMB)},
                    device_id_type=MESH,
                )
    payload[...] = jnp.zeros_like(payload)

    beta = hyper[0]
    gain = 1.0 - beta

    def prepare():
        wait(small)
        for l in range(n_layers):
            for k in range(3):
                for j in range(4):
                    old_a[l, k * 4 + j : k * 4 + j + 1, :] = rq[k, l : l + 1, j * 128 : (j + 1) * 128]
                for j in range(2):
                    old_ac[l, k * 2 + j : k * 2 + j + 1, :] = cq[k, l : l + 1, j * 128 : (j + 1) * 128]
            for j in range(2):
                old_b[l, j : j + 1, :] = ro[l : l + 1, j * 128 : (j + 1) * 128]
            for j in range(4):
                old_bc[l, j : j + 1, :] = co[l : l + 1, j * 128 : (j + 1) * 128]
        pl.semaphore_wait(barrier, ATT * EMB - 1)

    def zero(l):
        u_qkv[l] = jnp.zeros_like(u_qkv[l])
        u_out[l] = jnp.zeros_like(u_out[l])

    def mul_a(l, s):
        grads = jnp.concatenate([dyb[s, k] for k in range(3)], axis=1)
        prod = lax.dot_general(xb[s], grads, (((0,), (0,)), ((), ())), preferred_element_type=F32)
        for k in range(3):
            u_qkv[l, k] = u_qkv[l, k] + prod[:, k * 256 : (k + 1) * 256]

    def mul_b(l, s):
        prod = lax.dot_general(xab[s], dob[s], (((0,), (0,)), ((), ())), preferred_element_type=F32)
        u_out[l] = u_out[l] + prod

    def refill_a(g):
        @pl.when(g + NA < n_layers * nb)
        def _():
            start(copies_a(g + NA))

    def refill_b(g):
        @pl.when(g + NB < n_layers * nb)
        def _():
            start(copies_b(g + NB))

    def stats_a(l):
        for k in range(3):
            cols = None
            for q in range(2):
                g = u_qkv[l, k, pl.ds(q * 256, 256)]
                sq = g * g
                row_a[k, pl.ds(q * 256, 256)] = sq[:, :128] + sq[:, 128:]
                part = jnp.sum(sq, axis=0, keepdims=True)
                cols = part if cols is None else cols + part
            for j in range(2):
                emb_a[l, 0, k * 2 + j : k * 2 + j + 1, :] = cols[:, j * 128 : (j + 1) * 128]
        for k in range(3):
            rows = rows_to_lanes(row_a[k])
            for j in range(4):
                att_a[l, 0, k * 4 + j : k * 4 + j + 1, :] = rows[:, j * 128 : (j + 1) * 128]
        send_att(att_a, 0, l)
        send_emb(emb_a, 1, l)

    def stats_b(l):
        parts = []
        for q in range(2):
            g = u_out[l, :, pl.ds(q * 256, 256)]
            sq = g * g
            parts.append(sq[:, :128] + sq[:, 128:])
            cols = jnp.sum(sq, axis=0, keepdims=True)
            for j in range(2):
                att_b[l, 0, q * 2 + j : q * 2 + j + 1, :] = cols[:, j * 128 : (j + 1) * 128]
            if q == 0:
                row_b[...] = parts[0]
            else:
                row_b[...] = row_b[...] + parts[1]
        rows = rows_to_lanes(row_b[...])
        for j in range(2):
            emb_b[l, 0, j : j + 1, :] = rows[:, j * 128 : (j + 1) * 128]
        send_att(att_b, 2, l)
        send_emb(emb_b, 3, l)

    def record(slot, value):
        lane = lax.broadcasted_iota(jnp.int32, (1, 128), 1)
        payload[...] = jnp.where(lane == slot, value, payload[...])

    def sum_w(l):
        wait(copies_w(l))
        for k in range(3):
            w = wv_qkv[l, k]
            record(32 + l * 4 + k, total(fold8(w[:, :128] * w[:, :128] + w[:, 128:] * w[:, 128:])))
        w = wv_out[l]
        part = sum(fold8(w[:, j * 128 : (j + 1) * 128] * w[:, j * 128 : (j + 1) * 128]) for j in range(4))
        record(32 + l * 4 + 3, total(part))

    def apply_a(l):
        wait_group(att_a, ATT, 0, l)
        wait_group(emb_a, EMB, 1, l)
        row_sum = att_a[l, 0]
        for d in range(1, ATT):
            row_sum = row_sum + att_a[l, d]
        col_sum = emb_a[l, 0]
        for d in range(1, EMB):
            col_sum = col_sum + emb_a[l, d]
        r_new = beta * old_a[l] + gain * (row_sum * (1.0 / d_model) + EPS_SQUARE)
        c_new = beta * old_ac[l] + gain * (col_sum * (1.0 / d_model) + EPS_SQUARE)
        rn_qkv[l] = r_new
        cn_qkv[l] = c_new
        b_all = lax.rsqrt(c_new)
        for k in range(3):
            r_k = r_new[k * 4 : (k + 1) * 4]
            mean = total(r_k) * (1.0 / 512)
            a_k = lax.rsqrt(r_k / mean)
            tsum = jnp.zeros((8, 128), F32)
            for j in range(4):
                a_col = jnp.broadcast_to(a_k[j : j + 1], (128, 128)).T
                for h in range(2):
                    rr, cc = pl.ds(j * 128, 128), pl.ds(h * 128, 128)
                    u = u_qkv[l, k, rr, cc] * a_col * b_all[k * 2 + h : k * 2 + h + 1]
                    u_qkv[l, k, rr, cc] = u
                    tsum = tsum + fold8(u * u)
            record(l * 4 + k, total(tsum))
            record(16 + l * 4 + k, mean)

    def apply_b(l):
        wait_group(att_b, ATT, 2, l)
        wait_group(emb_b, EMB, 3, l)
        col_sum = att_b[l, 0]
        for d in range(1, ATT):
            col_sum = col_sum + att_b[l, d]
        row_sum = emb_b[l, 0]
        for d in range(1, EMB):
            row_sum = row_sum + emb_b[l, d]
        r_new = beta * old_b[l] + gain * (row_sum * (1.0 / d_model) + EPS_SQUARE)
        c_new = beta * old_bc[l] + gain * (col_sum * (1.0 / d_model) + EPS_SQUARE)
        b_all = lax.rsqrt(c_new)
        mean = total(r_new) * (1.0 / 256)
        a_all = lax.rsqrt(r_new / mean)
        tsum = jnp.zeros((8, 128), F32)
        for j in range(2):
            a_col = jnp.broadcast_to(a_all[j : j + 1], (128, 128)).T
            for h in range(4):
                rr, cc = pl.ds(j * 128, 128), pl.ds(h * 128, 128)
                u = u_out[l, rr, cc] * a_col * b_all[h : h + 1]
                u_out[l, rr, cc] = u
                tsum = tsum + fold8(u * u)
        rn_out[l] = r_new
        cn_out[l] = c_new
        record(l * 4 + 3, total(tsum))
        record(16 + l * 4 + 3, mean)

    last = n_layers - 1

    def layer(l, carry):
        zero(l)

        def block(i, carry):
            g = l * nb + i
            wait(copies_a(g))
            wait(copies_b(g))
            mul_a(l, g % NA)
            mul_b(l, g % NB)
            refill_a(g)
            refill_b(g)
            return carry

        lax.fori_loop(0, nb, block, 0)

        @pl.when(l == 0)
        def _():
            prepare()

        stats_a(l)
        stats_b(l)

        @pl.when(l > 0)
        def _():
            apply_a(l - 1)
            apply_b(l - 1)

        return carry

    lax.fori_loop(0, last, layer, 0)
    zero(last)

    def block_a(i, carry):
        g = last * nb + i
        wait(copies_a(g))
        mul_a(last, g % NA)
        return carry

    lax.fori_loop(0, nb, block_a, 0)
    for l in range(n_layers):
        start(copies_w(l))
    stats_a(last)

    def block_b(i, carry):
        g = last * nb + i
        wait(copies_b(g))
        mul_b(last, g % NB)
        return carry

    lax.fori_loop(0, nb, block_b, 0)
    stats_b(last)
    apply_a(last - 1)
    apply_b(last - 1)
    for l in range(n_layers):
        sum_w(l)
    apply_a(last)
    apply_b(last)

    glob[0] = payload[...]
    for da in (4, 3, 5, 2, 6, 1, 7, 0):
        for de in (2, 3, 1, 0):
            if da or de:
                pltpu.make_async_remote_copy(
                    src_ref=glob.at[0], dst_ref=glob.at[((ATT - da) % ATT) * EMB + (EMB - de) % EMB],
                    send_sem=send_g, recv_sem=recv_g,
                    device_id={"att": lax.rem(me_att + da, ATT), "emb": lax.rem(me_emb + de, EMB)},
                    device_id_type=MESH,
                ).start()
    others = glob.at[pl.ds(1, ATT * EMB - 1)]
    pltpu.make_async_copy(others, others, send_g).wait()
    pltpu.make_async_copy(others, others, recv_g).wait()
    n_dev = ATT * EMB
    mean_sum = jnp.zeros((1, 128), F32)
    w_sum = jnp.zeros((1, 128), F32)
    u_sum = jnp.zeros((1, 128), F32)
    for d in range(n_dev):
        row = glob[d]
        local_mean = pltpu.roll(row, 128 - 16, 1)
        mean_sum = mean_sum + local_mean
        w_sum = w_sum + pltpu.roll(row, 128 - 32, 1)
    mean_all = mean_sum * (1.0 / n_dev)
    for d in range(n_dev):
        row = glob[d]
        u_sum = u_sum + row * (mean_all / pltpu.roll(row, 128 - 16, 1))
    n_elems = float(d_model) * d_model
    rms_u = jnp.sqrt(u_sum * (1.0 / n_elems))
    rms_w = jnp.sqrt(w_sum * (1.0 / n_elems))
    step = hyper[1] * jnp.maximum(EPS_SCALE, rms_w) / jnp.maximum(1.0, rms_u / hyper[2])
    scales[...] = step * jnp.sqrt(mean_all / pltpu.roll(payload[...], 128 - 16, 1))


def write_kernel(
    n_layers, u_qkv, u_out, wv_qkv, wv_out, scales, rn_qkv, cn_qkv, rn_out, cn_out,
    wn_qkv, wn_out, r_qkv, c_qkv, r_out, c_out,
    st_a, st_b, st_rq, st_cq, st_r, st_c, sem_w, sem_s,
):
    for l in range(n_layers):
        for k in range(3):
            for j in range(4):
                st_rq[k, l : l + 1, j * 128 : (j + 1) * 128] = rn_qkv[l, k * 4 + j : k * 4 + j + 1]
            for j in range(2):
                st_cq[k, l : l + 1, j * 128 : (j + 1) * 128] = cn_qkv[l, k * 2 + j : k * 2 + j + 1]
        for j in range(2):
            st_r[l : l + 1, j * 128 : (j + 1) * 128] = rn_out[l, j : j + 1]
        for j in range(4):
            st_c[l : l + 1, j * 128 : (j + 1) * 128] = cn_out[l, j : j + 1]
    small = [
        pltpu.make_async_copy(src, dst, sem_s.at[n])
        for n, (src, dst) in enumerate(((st_rq, r_qkv), (st_cq, c_qkv), (st_r, r_out), (st_c, c_out)))
    ]
    for copy in small:
        copy.start()
    copies = []
    for l in range(n_layers):
        for k in range(4):
            m = l * 4 + k
            s = scales[0:1, m : m + 1]
            if k < 3:
                st_a[l, k] = wv_qkv[l, k] - s * u_qkv[l, k]
                copy = pltpu.make_async_copy(st_a.at[l, k], wn_qkv.at[l, k], sem_w.at[m])
            else:
                st_b[l] = wv_out[l] - s * u_out[l]
                copy = pltpu.make_async_copy(st_b.at[l], wn_out.at[l], sem_w.at[m])
            copy.start()
            copies.append(copy)
    for copy in copies + small:
        copy.wait()


def solution(mesh):
    att, emb = mesh.shape["att"], mesh.shape["emb"]
    qkv = P(None, None, "emb", "att")
    out = P(None, "att", "emb")
    row = P(None, None, "emb")
    col = P(None, None, "att")

    def local_run(w_qkv, w_out, x_in, dy_qkv, x_attn, dy_out, r_qkv, c_qkv, r_out, c_out, hyper_params):
        n_layers, n_tokens = x_in.shape[:2]
        d_model = x_in.shape[2] * emb
        hbm = pl.BlockSpec(memory_space=pltpu.HBM)
        vmem = pl.BlockSpec(memory_space=pltpu.VMEM)
        smem = pl.BlockSpec(memory_space=pltpu.SMEM)
        like = lambda x: jax.ShapeDtypeStruct(x.shape, x.dtype)
        kept = lambda x: pltpu.VMEM(x.shape, x.dtype)
        stat = lambda n: pltpu.VMEM((n_layers, n, 128), F32)
        r_qkv, c_qkv = jnp.swapaxes(r_qkv, 0, 1), jnp.swapaxes(c_qkv, 0, 1)
        mids = pl.pallas_call(
            functools.partial(step_kernel, n_layers, n_tokens, d_model),
            out_shape=(
                kept(w_qkv), kept(w_out), kept(w_qkv), kept(w_out), pltpu.VMEM((1, 128), F32),
                stat(12), stat(6), stat(2), stat(4),
            ),
            in_specs=[smem] + [hbm] * 10,
            out_specs=[vmem] * 9,
            scratch_shapes=[
                pltpu.VMEM((NA, TB, 512), BF16), pltpu.VMEM((NA, 3, TB, 256), BF16),
                pltpu.VMEM((NB, TB, 256), BF16), pltpu.VMEM((NB, TB, 512), BF16),
                pltpu.VMEM(r_qkv.shape, F32), pltpu.VMEM(c_qkv.shape, F32),
                pltpu.VMEM(r_out.shape, F32), pltpu.VMEM(c_out.shape, F32),
                pltpu.VMEM((3, 512, 128), F32), pltpu.VMEM((256, 128), F32),
                pltpu.VMEM((n_layers, ATT, 12, 128), F32), pltpu.VMEM((n_layers, EMB, 6, 128), F32),
                pltpu.VMEM((n_layers, ATT, 4, 128), F32), pltpu.VMEM((n_layers, EMB, 2, 128), F32),
                pltpu.VMEM((ATT * EMB, 1, 128), F32),
                pltpu.VMEM((n_layers, 12, 128), F32), pltpu.VMEM((n_layers, 6, 128), F32),
                pltpu.VMEM((n_layers, 2, 128), F32), pltpu.VMEM((n_layers, 4, 128), F32),
                pltpu.VMEM((1, 128), F32),
                pltpu.SemaphoreType.DMA((NA, 2)), pltpu.SemaphoreType.DMA((NB, 2)),
                pltpu.SemaphoreType.DMA((n_layers, 2)), pltpu.SemaphoreType.DMA((4,)),
                pltpu.SemaphoreType.DMA((4, n_layers)), pltpu.SemaphoreType.DMA((4, n_layers)),
                pltpu.SemaphoreType.DMA, pltpu.SemaphoreType.DMA,
            ],
            compiler_params=pltpu.CompilerParams(
                collective_id=0, has_side_effects=True, vmem_limit_bytes=45 * 2**20
            ),
            name="adafactor_step",
        )(hyper_params, x_in, dy_qkv, x_attn, dy_out, w_qkv, w_out, r_qkv, c_qkv, r_out, c_out)
        wn_qkv, wn_out, rn_qkv, cn_qkv, rn_out, cn_out = pl.pallas_call(
            functools.partial(write_kernel, n_layers),
            out_shape=(like(w_qkv), like(w_out), like(r_qkv), like(c_qkv), like(r_out), like(c_out)),
            in_specs=[vmem] * 9,
            out_specs=[hbm] * 6,
            scratch_shapes=[
                pltpu.VMEM(w_qkv.shape, F32), pltpu.VMEM(w_out.shape, F32),
                pltpu.VMEM(r_qkv.shape, F32), pltpu.VMEM(c_qkv.shape, F32),
                pltpu.VMEM(r_out.shape, F32), pltpu.VMEM(c_out.shape, F32),
                pltpu.SemaphoreType.DMA((4 * n_layers,)), pltpu.SemaphoreType.DMA((4,)),
            ],
            compiler_params=pltpu.CompilerParams(vmem_limit_bytes=16 * 2**20),
            name="adafactor_write",
        )(*mids)
        return wn_qkv, wn_out, jnp.swapaxes(rn_qkv, 0, 1), jnp.swapaxes(cn_qkv, 0, 1), rn_out, cn_out

    return jax.shard_map(
        local_run,
        mesh=mesh,
        in_specs=(qkv, out, row, P(None, None, None, "att"), col, row, row, col, P(None, "att"), P(None, "emb"), P()),
        out_specs=(qkv, out, row, col, P(None, "att"), P(None, "emb")),
        check_vma=False,
    )
```

```python
import functools

import jax
import jax.numpy as jnp
from jax import lax
from jax.experimental import pallas as pl
from jax.experimental.pallas import tpu as pltpu
from jax.sharding import PartitionSpec as P

EPS_SQUARE = 1e-30
EPS_SCALE = 1e-3
F32 = jnp.float32
BF16 = jnp.bfloat16
MESH = pl.DeviceIdType.MESH
TB = 2048
SUB = 2048
NA = 3
NB = 3
ATT = 8
EMB = 4


def rows_to_lanes(part):
    return jnp.sum(part.T, axis=0, keepdims=True)


def fold8(part):
    return jnp.sum(part.reshape(part.shape[0] // 8, 8, 128), axis=0)


def total(part):
    return jnp.sum(jnp.sum(part, axis=0, keepdims=True), axis=1, keepdims=True)


def step_kernel(
    n_layers, n_tokens, d_model,
    hyper, x_in, dy_qkv, x_attn, dy_out, w_qkv, w_out, r_qkv, c_qkv, r_out, c_out,
    u_qkv, u_out, wv_qkv, wv_out, scales, rn_qkv, cn_qkv, rn_out, cn_out,
    xb, dyb, xab, dob, rq, cq, ro, co, row_a, row_b,
    att_a, emb_a, att_b, emb_b, glob, old_a, old_ac, old_b, old_bc, payload,
    sem_a, sem_b, sem_w, sem_s, send_sem, recv_sem, send_g, recv_g,
):
    nb = n_tokens // TB
    me_att = lax.axis_index("att")
    me_emb = lax.axis_index("emb")

    def copies_a(g, subs=range(TB // SUB)):
        l, i, s = g // nb, g % nb, g % NA
        copies = []
        for n in subs:
            src = pl.ds(pl.multiple_of(i * TB + n * SUB, SUB), SUB)
            dst = pl.ds(n * SUB, SUB)
            copies.append(pltpu.make_async_copy(x_in.at[l, src], xb.at[s, dst], sem_a.at[s, 2 * n]))
            copies.append(pltpu.make_async_copy(dy_qkv.at[l, :, src], dyb.at[s, :, dst], sem_a.at[s, 2 * n + 1]))
        return copies

    def copies_b(g, subs=range(TB // SUB)):
        l, i, s = g // nb, g % nb, g % NB
        copies = []
        for n in subs:
            src = pl.ds(pl.multiple_of(i * TB + n * SUB, SUB), SUB)
            dst = pl.ds(n * SUB, SUB)
            copies.append(pltpu.make_async_copy(x_attn.at[l, src], xab.at[s, dst], sem_b.at[s, 2 * n]))
            copies.append(pltpu.make_async_copy(dy_out.at[l, src], dob.at[s, dst], sem_b.at[s, 2 * n + 1]))
        return copies

    def copies_w(l):
        return (
            pltpu.make_async_copy(w_qkv.at[l], wv_qkv.at[l], sem_w.at[l, 0]),
            pltpu.make_async_copy(w_out.at[l], wv_out.at[l], sem_w.at[l, 1]),
        )

    def start(copies):
        for copy in copies:
            copy.start()

    def wait(copies):
        for copy in copies:
            copy.wait()

    def send_att(buf, kind, l):
        for d in (4, 3, 5, 2, 6, 1, 7):
            pltpu.make_async_remote_copy(
                src_ref=buf.at[l, 0], dst_ref=buf.at[l, ATT - d],
                send_sem=send_sem.at[kind, l], recv_sem=recv_sem.at[kind, l],
                device_id={"att": lax.rem(me_att + d, ATT)}, device_id_type=MESH,
            ).start()

    def send_emb(buf, kind, l):
        for d in (2, 1, 3):
            pltpu.make_async_remote_copy(
                src_ref=buf.at[l, 0], dst_ref=buf.at[l, EMB - d],
                send_sem=send_sem.at[kind, l], recv_sem=recv_sem.at[kind, l],
                device_id={"emb": lax.rem(me_emb + d, EMB)}, device_id_type=MESH,
            ).start()

    def wait_group(buf, n, kind, l):
        others = buf.at[l, pl.ds(1, n - 1)]
        pltpu.make_async_copy(others, others, send_sem.at[kind, l]).wait()
        pltpu.make_async_copy(others, others, recv_sem.at[kind, l]).wait()

    small = [
        pltpu.make_async_copy(src, dst, sem_s.at[n])
        for n, (src, dst) in enumerate(((r_qkv, rq), (c_qkv, cq), (r_out, ro), (c_out, co)))
    ]
    start(small)
    for n in range(TB // SUB):
        start(copies_a(jnp.int32(0), (n,)))
        start(copies_b(jnp.int32(0), (n,)))
    for g in range(1, NA):
        start(copies_a(jnp.int32(g)))
        start(copies_b(jnp.int32(g)))

    barrier = pltpu.get_barrier_semaphore()
    for da in range(ATT):
        for de in range(EMB):
            if da or de:
                pl.semaphore_signal(
                    barrier, inc=1,
                    device_id={"att": lax.rem(me_att + da, ATT), "emb": lax.rem(me_emb + de, EMB)},
                    device_id_type=MESH,
                )
    payload[...] = jnp.zeros_like(payload)

    beta = hyper[0]
    gain = 1.0 - beta

    def prepare():
        wait(small)
        for l in range(n_layers):
            for k in range(3):
                for j in range(4):
                    old_a[l, k * 4 + j : k * 4 + j + 1, :] = rq[k, l : l + 1, j * 128 : (j + 1) * 128]
                for j in range(2):
                    old_ac[l, k * 2 + j : k * 2 + j + 1, :] = cq[k, l : l + 1, j * 128 : (j + 1) * 128]
            for j in range(2):
                old_b[l, j : j + 1, :] = ro[l : l + 1, j * 128 : (j + 1) * 128]
            for j in range(4):
                old_bc[l, j : j + 1, :] = co[l : l + 1, j * 128 : (j + 1) * 128]
        pl.semaphore_wait(barrier, ATT * EMB - 1)

    def mul_a(l, s, keep, part=slice(None)):
        grads = jnp.concatenate([dyb[s, k, part] for k in range(3)], axis=1)
        prod = lax.dot_general(xb[s, part], grads, (((0,), (0,)), ((), ())), preferred_element_type=F32)
        for k in range(3):
            u_qkv[l, k] = jnp.where(keep, u_qkv[l, k], 0.0) + prod[:, k * 256 : (k + 1) * 256]

    def mul_b(l, s, keep, part=slice(None)):
        prod = lax.dot_general(xab[s, part], dob[s, part], (((0,), (0,)), ((), ())), preferred_element_type=F32)
        u_out[l] = jnp.where(keep, u_out[l], 0.0) + prod

    def refill_a(g):
        @pl.when(g + NA < n_layers * nb)
        def _():
            start(copies_a(g + NA))

    def refill_b(g):
        @pl.when(g + NB < n_layers * nb)
        def _():
            start(copies_b(g + NB))

    def stats_a(l):
        for k in range(3):
            cols = None
            for q in range(2):
                g = u_qkv[l, k, pl.ds(q * 256, 256)]
                sq = g * g
                row_a[k, pl.ds(q * 256, 256)] = sq[:, :128] + sq[:, 128:]
                part = jnp.sum(sq, axis=0, keepdims=True)
                cols = part if cols is None else cols + part
            for j in range(2):
                emb_a[l, 0, k * 2 + j : k * 2 + j + 1, :] = cols[:, j * 128 : (j + 1) * 128]
        for k in range(3):
            rows = rows_to_lanes(row_a[k])
            for j in range(4):
                att_a[l, 0, k * 4 + j : k * 4 + j + 1, :] = rows[:, j * 128 : (j + 1) * 128]
        send_att(att_a, 0, l)
        send_emb(emb_a, 1, l)

    def stats_b(l):
        parts = []
        for q in range(2):
            g = u_out[l, :, pl.ds(q * 256, 256)]
            sq = g * g
            parts.append(sq[:, :128] + sq[:, 128:])
            cols = jnp.sum(sq, axis=0, keepdims=True)
            for j in range(2):
                att_b[l, 0, q * 2 + j : q * 2 + j + 1, :] = cols[:, j * 128 : (j + 1) * 128]
            if q == 0:
                row_b[...] = parts[0]
            else:
                row_b[...] = row_b[...] + parts[1]
        rows = rows_to_lanes(row_b[...])
        for j in range(2):
            emb_b[l, 0, j : j + 1, :] = rows[:, j * 128 : (j + 1) * 128]
        send_att(att_b, 2, l)
        send_emb(emb_b, 3, l)

    def record(slot, value):
        lane = lax.broadcasted_iota(jnp.int32, (1, 128), 1)
        payload[...] = jnp.where(lane == slot, value, payload[...])

    def sum_w(l):
        wait(copies_w(l))
        for k in range(3):
            w = wv_qkv[l, k]
            record(32 + l * 4 + k, total(fold8(w[:, :128] * w[:, :128] + w[:, 128:] * w[:, 128:])))
        w = wv_out[l]
        part = sum(fold8(w[:, j * 128 : (j + 1) * 128] * w[:, j * 128 : (j + 1) * 128]) for j in range(4))
        record(32 + l * 4 + 3, total(part))

    def apply_a(l):
        row_sum = att_a[l, 0]
        for d in range(1, ATT):
            row_sum = row_sum + att_a[l, d]
        col_sum = emb_a[l, 0]
        for d in range(1, EMB):
            col_sum = col_sum + emb_a[l, d]
        r_new = beta * old_a[l] + gain * (row_sum * (1.0 / d_model) + EPS_SQUARE)
        c_new = beta * old_ac[l] + gain * (col_sum * (1.0 / d_model) + EPS_SQUARE)
        rn_qkv[l] = r_new
        cn_qkv[l] = c_new
        b_all = lax.rsqrt(c_new)
        for k in range(3):
            r_k = r_new[k * 4 : (k + 1) * 4]
            mean = total(r_k) * (1.0 / 512)
            a_k = lax.rsqrt(r_k / mean)
            tsum = jnp.zeros((8, 128), F32)
            for j in range(4):
                a_col = jnp.broadcast_to(a_k[j : j + 1], (128, 128)).T
                for h in range(2):
                    rr, cc = pl.ds(j * 128, 128), pl.ds(h * 128, 128)
                    u = u_qkv[l, k, rr, cc] * a_col * b_all[k * 2 + h : k * 2 + h + 1]
                    u_qkv[l, k, rr, cc] = u
                    tsum = tsum + fold8(u * u)
            record(l * 4 + k, total(tsum) / mean)
            record(16 + l * 4 + k, mean)

    def apply_b(l):
        col_sum = att_b[l, 0]
        for d in range(1, ATT):
            col_sum = col_sum + att_b[l, d]
        row_sum = emb_b[l, 0]
        for d in range(1, EMB):
            row_sum = row_sum + emb_b[l, d]
        r_new = beta * old_b[l] + gain * (row_sum * (1.0 / d_model) + EPS_SQUARE)
        c_new = beta * old_bc[l] + gain * (col_sum * (1.0 / d_model) + EPS_SQUARE)
        b_all = lax.rsqrt(c_new)
        mean = total(r_new) * (1.0 / 256)
        a_all = lax.rsqrt(r_new / mean)
        tsum = jnp.zeros((8, 128), F32)
        for j in range(2):
            a_col = jnp.broadcast_to(a_all[j : j + 1], (128, 128)).T
            for h in range(4):
                rr, cc = pl.ds(j * 128, 128), pl.ds(h * 128, 128)
                u = u_out[l, rr, cc] * a_col * b_all[h : h + 1]
                u_out[l, rr, cc] = u
                tsum = tsum + fold8(u * u)
        rn_out[l] = r_new
        cn_out[l] = c_new
        record(l * 4 + 3, total(tsum) / mean)
        record(16 + l * 4 + 3, mean)

    last = n_layers - 1

    def arrive_a(l):
        wait_group(att_a, ATT, 0, l)
        wait_group(emb_a, EMB, 1, l)

    def arrive_b(l):
        wait_group(att_b, ATT, 2, l)
        wait_group(emb_b, EMB, 3, l)

    def piece(n, carry):
        part = pl.ds(pl.multiple_of(n * SUB, SUB), SUB)
        for m in range(TB // SUB):
            @pl.when(n == m)
            def _():
                wait(copies_a(jnp.int32(0), (m,)))
                wait(copies_b(jnp.int32(0), (m,)))

        mul_a(0, 0, n > 0, part)
        mul_b(0, 0, n > 0, part)
        return carry

    lax.fori_loop(0, TB // SUB, piece, 0)
    refill_a(jnp.int32(0))
    refill_b(jnp.int32(0))

    def layer(l, carry):
        def block(i, carry):
            g = l * nb + i
            wait(copies_a(g))
            wait(copies_b(g))
            mul_a(l, g % NA, i > 0)
            mul_b(l, g % NB, i > 0)
            refill_a(g)
            refill_b(g)
            return carry

        lax.fori_loop(jnp.where(l == 0, 1, 0), nb, block, 0)

        @pl.when(l == 0)
        def _():
            prepare()

        stats_a(l)
        stats_b(l)
        return carry

    lax.fori_loop(0, last, layer, 0)

    def block_a(i, carry):
        g = last * nb + i
        wait(copies_a(g))
        mul_a(last, g % NA, i > 0)
        return carry

    lax.fori_loop(0, nb, block_a, 0)
    for l in range(n_layers):
        start(copies_w(l))
    stats_a(last)

    def block_b(i, carry):
        g = last * nb + i
        wait(copies_b(g))
        mul_b(last, g % NB, i > 0)
        return carry

    lax.fori_loop(0, nb, block_b, 0)
    stats_b(last)

    def earlier(l, carry):
        arrive_a(l)
        arrive_b(l)
        apply_a(l)
        apply_b(l)
        return carry

    lax.fori_loop(0, last, earlier, 0)

    def weights(l, carry):
        sum_w(l)
        return carry

    lax.fori_loop(0, n_layers, weights, 0)
    arrive_a(last)
    apply_a(last)
    arrive_b(last)
    apply_b(last)

    glob[0] = payload[...]
    for da in (4, 3, 5, 2, 6, 1, 7, 0):
        for de in (2, 3, 1, 0):
            if da or de:
                pltpu.make_async_remote_copy(
                    src_ref=glob.at[0], dst_ref=glob.at[((ATT - da) % ATT) * EMB + (EMB - de) % EMB],
                    send_sem=send_g, recv_sem=recv_g,
                    device_id={"att": lax.rem(me_att + da, ATT), "emb": lax.rem(me_emb + de, EMB)},
                    device_id_type=MESH,
                ).start()
    others = glob.at[pl.ds(1, ATT * EMB - 1)]
    pltpu.make_async_copy(others, others, send_g).wait()
    pltpu.make_async_copy(others, others, recv_g).wait()
    n_dev = ATT * EMB
    sums = glob[0]
    for d in range(1, n_dev):
        sums = sums + glob[d]
    mean_all = pltpu.roll(sums, 128 - 16, 1) * (1.0 / n_dev)
    w_sum = pltpu.roll(sums, 128 - 32, 1)
    u_sum = sums * mean_all
    n_elems = float(d_model) * d_model
    rms_u = jnp.sqrt(u_sum * (1.0 / n_elems))
    rms_w = jnp.sqrt(w_sum * (1.0 / n_elems))
    step = hyper[1] * jnp.maximum(EPS_SCALE, rms_w) / jnp.maximum(1.0, rms_u / hyper[2])
    scales[...] = step * jnp.sqrt(mean_all / pltpu.roll(payload[...], 128 - 16, 1))


def write_kernel(
    n_layers, u_qkv, u_out, wv_qkv, wv_out, scales, rn_qkv, cn_qkv, rn_out, cn_out,
    wn_qkv, wn_out, r_qkv, c_qkv, r_out, c_out,
    st_a, st_b, st_rq, st_cq, st_r, st_c, sem_w, sem_s,
):
    copies = []
    for l in range(n_layers):
        for k in range(4):
            m = l * 4 + k
            s = scales[0:1, m : m + 1]
            parts = 4 if m == 0 else 1
            for n in range(parts):
                if k < 3:
                    rows = pl.ds(n * (512 // parts), 512 // parts)
                    st_a[l, k, rows] = wv_qkv[l, k, rows] - s * u_qkv[l, k, rows]
                    copy = pltpu.make_async_copy(st_a.at[l, k, rows], wn_qkv.at[l, k, rows], sem_w.at[m if n == 0 else 15 + n])
                else:
                    st_b[l] = wv_out[l] - s * u_out[l]
                    copy = pltpu.make_async_copy(st_b.at[l], wn_out.at[l], sem_w.at[m])
                copy.start()
                copies.append(copy)
    for l in range(n_layers):
        for k in range(3):
            for j in range(4):
                st_rq[k, l : l + 1, j * 128 : (j + 1) * 128] = rn_qkv[l, k * 4 + j : k * 4 + j + 1]
            for j in range(2):
                st_cq[k, l : l + 1, j * 128 : (j + 1) * 128] = cn_qkv[l, k * 2 + j : k * 2 + j + 1]
        for j in range(2):
            st_r[l : l + 1, j * 128 : (j + 1) * 128] = rn_out[l, j : j + 1]
        for j in range(4):
            st_c[l : l + 1, j * 128 : (j + 1) * 128] = cn_out[l, j : j + 1]
    small = [
        pltpu.make_async_copy(src, dst, sem_s.at[n])
        for n, (src, dst) in enumerate(((st_rq, r_qkv), (st_cq, c_qkv), (st_r, r_out), (st_c, c_out)))
    ]
    for copy in small:
        copy.start()
    for copy in copies + small:
        copy.wait()


def solution(mesh):
    att, emb = mesh.shape["att"], mesh.shape["emb"]
    qkv = P(None, None, "emb", "att")
    out = P(None, "att", "emb")
    row = P(None, None, "emb")
    col = P(None, None, "att")

    def local_run(w_qkv, w_out, x_in, dy_qkv, x_attn, dy_out, r_qkv, c_qkv, r_out, c_out, hyper_params):
        n_layers, n_tokens = x_in.shape[:2]
        d_model = x_in.shape[2] * emb
        hbm = pl.BlockSpec(memory_space=pltpu.HBM)
        vmem = pl.BlockSpec(memory_space=pltpu.VMEM)
        smem = pl.BlockSpec(memory_space=pltpu.SMEM)
        like = lambda x: jax.ShapeDtypeStruct(x.shape, x.dtype)
        kept = lambda x: pltpu.VMEM(x.shape, x.dtype)
        stat = lambda n: pltpu.VMEM((n_layers, n, 128), F32)
        r_qkv, c_qkv = jnp.swapaxes(r_qkv, 0, 1), jnp.swapaxes(c_qkv, 0, 1)
        mids = pl.pallas_call(
            functools.partial(step_kernel, n_layers, n_tokens, d_model),
            out_shape=(
                kept(w_qkv), kept(w_out), kept(w_qkv), kept(w_out), pltpu.VMEM((1, 128), F32),
                stat(12), stat(6), stat(2), stat(4),
            ),
            in_specs=[smem] + [hbm] * 10,
            out_specs=[vmem] * 9,
            scratch_shapes=[
                pltpu.VMEM((NA, TB, 512), BF16), pltpu.VMEM((NA, 3, TB, 256), BF16),
                pltpu.VMEM((NB, TB, 256), BF16), pltpu.VMEM((NB, TB, 512), BF16),
                pltpu.VMEM(r_qkv.shape, F32), pltpu.VMEM(c_qkv.shape, F32),
                pltpu.VMEM(r_out.shape, F32), pltpu.VMEM(c_out.shape, F32),
                pltpu.VMEM((3, 512, 128), F32), pltpu.VMEM((256, 128), F32),
                pltpu.VMEM((n_layers, ATT, 12, 128), F32), pltpu.VMEM((n_layers, EMB, 6, 128), F32),
                pltpu.VMEM((n_layers, ATT, 4, 128), F32), pltpu.VMEM((n_layers, EMB, 2, 128), F32),
                pltpu.VMEM((ATT * EMB, 1, 128), F32),
                pltpu.VMEM((n_layers, 12, 128), F32), pltpu.VMEM((n_layers, 6, 128), F32),
                pltpu.VMEM((n_layers, 2, 128), F32), pltpu.VMEM((n_layers, 4, 128), F32),
                pltpu.VMEM((1, 128), F32),
                pltpu.SemaphoreType.DMA((NA, 2 * TB // SUB)), pltpu.SemaphoreType.DMA((NB, 2 * TB // SUB)),
                pltpu.SemaphoreType.DMA((n_layers, 2)), pltpu.SemaphoreType.DMA((4,)),
                pltpu.SemaphoreType.DMA((4, n_layers)), pltpu.SemaphoreType.DMA((4, n_layers)),
                pltpu.SemaphoreType.DMA, pltpu.SemaphoreType.DMA,
            ],
            compiler_params=pltpu.CompilerParams(
                collective_id=0, has_side_effects=True, vmem_limit_bytes=45 * 2**20
            ),
            name="adafactor_step",
        )(hyper_params, x_in, dy_qkv, x_attn, dy_out, w_qkv, w_out, r_qkv, c_qkv, r_out, c_out)
        wn_qkv, wn_out, rn_qkv, cn_qkv, rn_out, cn_out = pl.pallas_call(
            functools.partial(write_kernel, n_layers),
            out_shape=(like(w_qkv), like(w_out), like(r_qkv), like(c_qkv), like(r_out), like(c_out)),
            in_specs=[vmem] * 9,
            out_specs=[hbm] * 6,
            scratch_shapes=[
                pltpu.VMEM(w_qkv.shape, F32), pltpu.VMEM(w_out.shape, F32),
                pltpu.VMEM(r_qkv.shape, F32), pltpu.VMEM(c_qkv.shape, F32),
                pltpu.VMEM(r_out.shape, F32), pltpu.VMEM(c_out.shape, F32),
                pltpu.SemaphoreType.DMA((4 * n_layers + 3,)), pltpu.SemaphoreType.DMA((4,)),
            ],
            compiler_params=pltpu.CompilerParams(vmem_limit_bytes=16 * 2**20),
            name="adafactor_write",
        )(*mids)
        return wn_qkv, wn_out, jnp.swapaxes(rn_qkv, 0, 1), jnp.swapaxes(cn_qkv, 0, 1), rn_out, cn_out

    return jax.shard_map(
        local_run,
        mesh=mesh,
        in_specs=(qkv, out, row, P(None, None, None, "att"), col, row, row, col, P(None, "att"), P(None, "emb"), P()),
        out_specs=(qkv, out, row, col, P(None, "att"), P(None, "emb")),
        check_vma=False,
    )
```

```python
import functools

import jax
import jax.numpy as jnp
from jax import lax
from jax.experimental import pallas as pl
from jax.experimental.pallas import tpu as pltpu
from jax.sharding import PartitionSpec as P

EPS_SQUARE = 1e-30
EPS_SCALE = 1e-3
F32 = jnp.float32
BF16 = jnp.bfloat16
MESH = pl.DeviceIdType.MESH
TB = 2048
SUB = 2048
NA = 3
NB = 3
ATT = 8
EMB = 4


def rows_to_lanes(part):
    return jnp.sum(part.T, axis=0, keepdims=True)


def fold8(part):
    return jnp.sum(part.reshape(part.shape[0] // 8, 8, 128), axis=0)


def total(part):
    return jnp.sum(jnp.sum(part, axis=0, keepdims=True), axis=1, keepdims=True)


def step_kernel(
    n_layers, n_tokens, d_model,
    hyper, x_in, dy_qkv, x_attn, dy_out, w_qkv, w_out, r_qkv, c_qkv, r_out, c_out,
    u_qkv, u_out, wv_qkv, wv_out, scales, rn_qkv, cn_qkv, rn_out, cn_out,
    xb, dyb, xab, dob, rq, cq, ro, co, row_a, row_b, a_cols, parts,
    att_a, emb_a, att_b, emb_b, glob, old_a, old_ac, old_b, old_bc, payload,
    sem_a, sem_b, sem_w, sem_s, send_sem, recv_sem, send_g, recv_g,
):
    nb = n_tokens // TB
    me_att = lax.axis_index("att")
    me_emb = lax.axis_index("emb")

    def copies_a(g, subs=range(TB // SUB)):
        l, i, s = g // nb, g % nb, g % NA
        copies = []
        for n in subs:
            src = pl.ds(pl.multiple_of(i * TB + n * SUB, SUB), SUB)
            dst = pl.ds(n * SUB, SUB)
            copies.append(pltpu.make_async_copy(x_in.at[l, src], xb.at[s, dst], sem_a.at[s, 2 * n]))
            copies.append(pltpu.make_async_copy(dy_qkv.at[l, :, src], dyb.at[s, :, dst], sem_a.at[s, 2 * n + 1]))
        return copies

    def copies_b(g, subs=range(TB // SUB)):
        l, i, s = g // nb, g % nb, g % NB
        copies = []
        for n in subs:
            src = pl.ds(pl.multiple_of(i * TB + n * SUB, SUB), SUB)
            dst = pl.ds(n * SUB, SUB)
            copies.append(pltpu.make_async_copy(x_attn.at[l, src], xab.at[s, dst], sem_b.at[s, 2 * n]))
            copies.append(pltpu.make_async_copy(dy_out.at[l, src], dob.at[s, dst], sem_b.at[s, 2 * n + 1]))
        return copies

    def copies_w(l):
        return (
            pltpu.make_async_copy(w_qkv.at[l], wv_qkv.at[l], sem_w.at[l, 0]),
            pltpu.make_async_copy(w_out.at[l], wv_out.at[l], sem_w.at[l, 1]),
        )

    def start(copies):
        for copy in copies:
            copy.start()

    def wait(copies):
        for copy in copies:
            copy.wait()

    def send_att(buf, kind, l):
        for d in (4, 3, 5, 2, 6, 1, 7):
            pltpu.make_async_remote_copy(
                src_ref=buf.at[l, 0], dst_ref=buf.at[l, ATT - d],
                send_sem=send_sem.at[kind, l], recv_sem=recv_sem.at[kind, l],
                device_id={"att": lax.rem(me_att + d, ATT)}, device_id_type=MESH,
            ).start()

    def send_emb(buf, kind, l):
        for d in (2, 1, 3):
            pltpu.make_async_remote_copy(
                src_ref=buf.at[l, 0], dst_ref=buf.at[l, EMB - d],
                send_sem=send_sem.at[kind, l], recv_sem=recv_sem.at[kind, l],
                device_id={"emb": lax.rem(me_emb + d, EMB)}, device_id_type=MESH,
            ).start()

    def wait_group(buf, n, kind, l):
        others = buf.at[l, pl.ds(1, n - 1)]
        pltpu.make_async_copy(others, others, send_sem.at[kind, l]).wait()
        pltpu.make_async_copy(others, others, recv_sem.at[kind, l]).wait()

    small = [
        pltpu.make_async_copy(src, dst, sem_s.at[n])
        for n, (src, dst) in enumerate(((r_qkv, rq), (c_qkv, cq), (r_out, ro), (c_out, co)))
    ]
    start(small)
    for n in range(TB // SUB):
        start(copies_a(jnp.int32(0), (n,)))
        start(copies_b(jnp.int32(0), (n,)))
    for g in range(1, NA):
        start(copies_a(jnp.int32(g)))
        start(copies_b(jnp.int32(g)))

    barrier = pltpu.get_barrier_semaphore()
    for da in range(ATT):
        for de in range(EMB):
            if da or de:
                pl.semaphore_signal(
                    barrier, inc=1,
                    device_id={"att": lax.rem(me_att + da, ATT), "emb": lax.rem(me_emb + de, EMB)},
                    device_id_type=MESH,
                )
    payload[...] = jnp.zeros_like(payload)

    beta = hyper[0]
    gain = 1.0 - beta

    def prepare():
        wait(small)
        for l in range(n_layers):
            for k in range(3):
                for j in range(4):
                    old_a[l, k * 4 + j : k * 4 + j + 1, :] = rq[k, l : l + 1, j * 128 : (j + 1) * 128]
                for j in range(2):
                    old_ac[l, k * 2 + j : k * 2 + j + 1, :] = cq[k, l : l + 1, j * 128 : (j + 1) * 128]
            for j in range(2):
                old_b[l, j : j + 1, :] = ro[l : l + 1, j * 128 : (j + 1) * 128]
            for j in range(4):
                old_bc[l, j : j + 1, :] = co[l : l + 1, j * 128 : (j + 1) * 128]
        pl.semaphore_wait(barrier, ATT * EMB - 1)

    def mul_a(l, s, keep, part=slice(None)):
        grads = jnp.concatenate([dyb[s, k, part] for k in range(3)], axis=1)
        prod = lax.dot_general(xb[s, part], grads, (((0,), (0,)), ((), ())), preferred_element_type=F32)
        for k in range(3):
            u_qkv[l, k] = jnp.where(keep, u_qkv[l, k], 0.0) + prod[:, k * 256 : (k + 1) * 256]

    def mul_b(l, s, keep, part=slice(None)):
        prod = lax.dot_general(xab[s, part], dob[s, part], (((0,), (0,)), ((), ())), preferred_element_type=F32)
        u_out[l] = jnp.where(keep, u_out[l], 0.0) + prod

    def refill_a(g):
        @pl.when(g + NA < n_layers * nb)
        def _():
            start(copies_a(g + NA))

    def refill_b(g):
        @pl.when(g + NB < n_layers * nb)
        def _():
            start(copies_b(g + NB))

    def stats_a(l):
        for k in range(3):
            cols = None
            for q in range(2):
                g = u_qkv[l, k, pl.ds(q * 256, 256)]
                sq = g * g
                row_a[k, pl.ds(q * 256, 256)] = sq[:, :128] + sq[:, 128:]
                part = jnp.sum(sq, axis=0, keepdims=True)
                cols = part if cols is None else cols + part
            for j in range(2):
                emb_a[l, 0, k * 2 + j : k * 2 + j + 1, :] = cols[:, j * 128 : (j + 1) * 128]
        for k in range(3):
            rows = rows_to_lanes(row_a[k])
            for j in range(4):
                att_a[l, 0, k * 4 + j : k * 4 + j + 1, :] = rows[:, j * 128 : (j + 1) * 128]
        send_att(att_a, 0, l)
        send_emb(emb_a, 1, l)

    def stats_b(l):
        parts = []
        for q in range(2):
            g = u_out[l, :, pl.ds(q * 256, 256)]
            sq = g * g
            parts.append(sq[:, :128] + sq[:, 128:])
            cols = jnp.sum(sq, axis=0, keepdims=True)
            for j in range(2):
                att_b[l, 0, q * 2 + j : q * 2 + j + 1, :] = cols[:, j * 128 : (j + 1) * 128]
            if q == 0:
                row_b[...] = parts[0]
            else:
                row_b[...] = row_b[...] + parts[1]
        rows = rows_to_lanes(row_b[...])
        for j in range(2):
            emb_b[l, 0, j : j + 1, :] = rows[:, j * 128 : (j + 1) * 128]
        send_att(att_b, 2, l)
        send_emb(emb_b, 3, l)

    def record(slot, value):
        lane = lax.broadcasted_iota(jnp.int32, (1, 128), 1)
        payload[...] = jnp.where(lane == 8 * slot, value, payload[...])

    def sum_w(l):
        wait(copies_w(l))
        for k in range(3):
            w = wv_qkv[l, k]
            parts[1, l * 4 + k] = fold8(w[:, :128] * w[:, :128] + w[:, 128:] * w[:, 128:])
        w = wv_out[l]
        parts[1, l * 4 + 3] = sum(fold8(w[:, j * 128 : (j + 1) * 128] * w[:, j * 128 : (j + 1) * 128]) for j in range(4))

    def apply_a(l):
        row_sum = att_a[l, 0]
        for d in range(1, ATT):
            row_sum = row_sum + att_a[l, d]
        col_sum = emb_a[l, 0]
        for d in range(1, EMB):
            col_sum = col_sum + emb_a[l, d]
        r_new = beta * old_a[l] + gain * (row_sum * (1.0 / d_model) + EPS_SQUARE)
        c_new = beta * old_ac[l] + gain * (col_sum * (1.0 / d_model) + EPS_SQUARE)
        rn_qkv[l] = r_new
        cn_qkv[l] = c_new
        b_all = lax.rsqrt(c_new)
        means = [total(r_new[k * 4 : (k + 1) * 4]) * (1.0 / 512) for k in range(3)]
        for k in range(3):
            a_k = lax.rsqrt(r_new[k * 4 : (k + 1) * 4] / means[k])
            for j in range(4):
                a_cols[k * 4 + j] = jnp.broadcast_to(a_k[j : j + 1], (128, 128)).T
        for k in range(3):
            tsum = jnp.zeros((8, 128), F32)
            for j in range(4):
                a_col = a_cols[k * 4 + j]
                for h in range(2):
                    rr, cc = pl.ds(j * 128, 128), pl.ds(h * 128, 128)
                    u = u_qkv[l, k, rr, cc] * a_col * b_all[k * 2 + h : k * 2 + h + 1]
                    u_qkv[l, k, rr, cc] = u
                    tsum = tsum + fold8(u * u)
            parts[0, l * 4 + k] = tsum
            record(l * 4 + k, means[k])

    def apply_b(l):
        col_sum = att_b[l, 0]
        for d in range(1, ATT):
            col_sum = col_sum + att_b[l, d]
        row_sum = emb_b[l, 0]
        for d in range(1, EMB):
            row_sum = row_sum + emb_b[l, d]
        r_new = beta * old_b[l] + gain * (row_sum * (1.0 / d_model) + EPS_SQUARE)
        c_new = beta * old_bc[l] + gain * (col_sum * (1.0 / d_model) + EPS_SQUARE)
        b_all = lax.rsqrt(c_new)
        mean = total(r_new) * (1.0 / 256)
        a_all = lax.rsqrt(r_new / mean)
        tsum = jnp.zeros((8, 128), F32)
        for j in range(2):
            a_col = jnp.broadcast_to(a_all[j : j + 1], (128, 128)).T
            for h in range(4):
                rr, cc = pl.ds(j * 128, 128), pl.ds(h * 128, 128)
                u = u_out[l, rr, cc] * a_col * b_all[h : h + 1]
                u_out[l, rr, cc] = u
                tsum = tsum + fold8(u * u)
        rn_out[l] = r_new
        cn_out[l] = c_new
        parts[0, l * 4 + 3] = tsum
        record(l * 4 + 3, mean)

    last = n_layers - 1

    def per_matrix(n):
        sums = rows_to_lanes(parts[n].reshape(128, 128))
        for shift in (4, 2, 1):
            sums = sums + pltpu.roll(sums, 128 - shift, 1)
        return sums

    def arrive_a(l):
        wait_group(att_a, ATT, 0, l)
        wait_group(emb_a, EMB, 1, l)

    def arrive_b(l):
        wait_group(att_b, ATT, 2, l)
        wait_group(emb_b, EMB, 3, l)

    def piece(n, carry):
        part = pl.ds(pl.multiple_of(n * SUB, SUB), SUB)
        for m in range(TB // SUB):
            @pl.when(n == m)
            def _():
                wait(copies_a(jnp.int32(0), (m,)))
                wait(copies_b(jnp.int32(0), (m,)))

        mul_a(0, 0, n > 0, part)
        mul_b(0, 0, n > 0, part)
        return carry

    lax.fori_loop(0, TB // SUB, piece, 0)
    refill_a(jnp.int32(0))
    refill_b(jnp.int32(0))

    def layer(l, carry):
        def block(i, carry):
            g = l * nb + i
            wait(copies_a(g))
            wait(copies_b(g))
            mul_a(l, g % NA, i > 0)
            mul_b(l, g % NB, i > 0)
            refill_a(g)
            refill_b(g)
            return carry

        lax.fori_loop(jnp.where(l == 0, 1, 0), nb, block, 0)

        @pl.when(l == 0)
        def _():
            prepare()

        stats_a(l)
        stats_b(l)
        return carry

    lax.fori_loop(0, last, layer, 0)

    def block_a(i, carry):
        g = last * nb + i
        wait(copies_a(g))
        mul_a(last, g % NA, i > 0)
        return carry

    lax.fori_loop(0, nb, block_a, 0)
    for l in range(n_layers):
        start(copies_w(l))
    stats_a(last)

    def block_b(i, carry):
        g = last * nb + i
        wait(copies_b(g))
        mul_b(last, g % NB, i > 0)
        return carry

    lax.fori_loop(0, nb, block_b, 0)
    stats_b(last)

    def earlier(l, carry):
        arrive_a(l)
        arrive_b(l)
        apply_a(l)
        apply_b(l)
        return carry

    lax.fori_loop(0, last, earlier, 0)

    def weights(l, carry):
        sum_w(l)
        return carry

    lax.fori_loop(0, n_layers, weights, 0)
    arrive_a(last)
    apply_a(last)
    w_parts = per_matrix(1)
    arrive_b(last)
    apply_b(last)

    phase = lax.broadcasted_iota(jnp.int32, (1, 128), 1) & 7
    row = jnp.where(phase == 1, pltpu.roll(w_parts, 1, 1), pltpu.roll(payload[...], 2, 1))
    glob[0] = jnp.where(phase == 0, per_matrix(0) / payload[...], row)
    for da in (4, 3, 5, 2, 6, 1, 7, 0):
        for de in (2, 3, 1, 0):
            if da or de:
                pltpu.make_async_remote_copy(
                    src_ref=glob.at[0], dst_ref=glob.at[((ATT - da) % ATT) * EMB + (EMB - de) % EMB],
                    send_sem=send_g, recv_sem=recv_g,
                    device_id={"att": lax.rem(me_att + da, ATT), "emb": lax.rem(me_emb + de, EMB)},
                    device_id_type=MESH,
                ).start()
    others = glob.at[pl.ds(1, ATT * EMB - 1)]
    pltpu.make_async_copy(others, others, send_g).wait()
    pltpu.make_async_copy(others, others, recv_g).wait()
    n_dev = ATT * EMB
    sums = glob[0]
    for d in range(1, n_dev):
        sums = sums + glob[d]
    mean_all = pltpu.roll(sums, 128 - 2, 1) * (1.0 / n_dev)
    w_sum = pltpu.roll(sums, 128 - 1, 1)
    u_sum = sums * mean_all
    n_elems = float(d_model) * d_model
    rms_u = jnp.sqrt(u_sum * (1.0 / n_elems))
    rms_w = jnp.sqrt(w_sum * (1.0 / n_elems))
    step = hyper[1] * jnp.maximum(EPS_SCALE, rms_w) / jnp.maximum(1.0, rms_u / hyper[2])
    scales[...] = step * jnp.sqrt(mean_all / payload[...])


def write_kernel(
    n_layers, u_qkv, u_out, wv_qkv, wv_out, scales, rn_qkv, cn_qkv, rn_out, cn_out,
    wn_qkv, wn_out, r_qkv, c_qkv, r_out, c_out,
    st_a, st_b, st_rq, st_cq, st_r, st_c, sem_w, sem_s,
):
    copies = []
    for l in range(n_layers):
        for k in range(4):
            m = l * 4 + k
            s = scales[0:1, 8 * m : 8 * m + 1]
            parts = 4 if m == 0 else 1
            for n in range(parts):
                if k < 3:
                    rows = pl.ds(n * (512 // parts), 512 // parts)
                    st_a[l, k, rows] = wv_qkv[l, k, rows] - s * u_qkv[l, k, rows]
                    copy = pltpu.make_async_copy(st_a.at[l, k, rows], wn_qkv.at[l, k, rows], sem_w.at[m if n == 0 else 15 + n])
                else:
                    st_b[l] = wv_out[l] - s * u_out[l]
                    copy = pltpu.make_async_copy(st_b.at[l], wn_out.at[l], sem_w.at[m])
                copy.start()
                copies.append(copy)
    for l in range(n_layers):
        for k in range(3):
            for j in range(4):
                st_rq[k, l : l + 1, j * 128 : (j + 1) * 128] = rn_qkv[l, k * 4 + j : k * 4 + j + 1]
            for j in range(2):
                st_cq[k, l : l + 1, j * 128 : (j + 1) * 128] = cn_qkv[l, k * 2 + j : k * 2 + j + 1]
        for j in range(2):
            st_r[l : l + 1, j * 128 : (j + 1) * 128] = rn_out[l, j : j + 1]
        for j in range(4):
            st_c[l : l + 1, j * 128 : (j + 1) * 128] = cn_out[l, j : j + 1]
    small = [
        pltpu.make_async_copy(src, dst, sem_s.at[n])
        for n, (src, dst) in enumerate(((st_rq, r_qkv), (st_cq, c_qkv), (st_r, r_out), (st_c, c_out)))
    ]
    for copy in small:
        copy.start()
    for copy in copies + small:
        copy.wait()


def solution(mesh):
    att, emb = mesh.shape["att"], mesh.shape["emb"]
    qkv = P(None, None, "emb", "att")
    out = P(None, "att", "emb")
    row = P(None, None, "emb")
    col = P(None, None, "att")

    def local_run(w_qkv, w_out, x_in, dy_qkv, x_attn, dy_out, r_qkv, c_qkv, r_out, c_out, hyper_params):
        n_layers, n_tokens = x_in.shape[:2]
        d_model = x_in.shape[2] * emb
        hbm = pl.BlockSpec(memory_space=pltpu.HBM)
        vmem = pl.BlockSpec(memory_space=pltpu.VMEM)
        smem = pl.BlockSpec(memory_space=pltpu.SMEM)
        like = lambda x: jax.ShapeDtypeStruct(x.shape, x.dtype)
        kept = lambda x: pltpu.VMEM(x.shape, x.dtype)
        stat = lambda n: pltpu.VMEM((n_layers, n, 128), F32)
        r_qkv, c_qkv = jnp.swapaxes(r_qkv, 0, 1), jnp.swapaxes(c_qkv, 0, 1)
        mids = pl.pallas_call(
            functools.partial(step_kernel, n_layers, n_tokens, d_model),
            out_shape=(
                kept(w_qkv), kept(w_out), kept(w_qkv), kept(w_out), pltpu.VMEM((1, 128), F32),
                stat(12), stat(6), stat(2), stat(4),
            ),
            in_specs=[smem] + [hbm] * 10,
            out_specs=[vmem] * 9,
            scratch_shapes=[
                pltpu.VMEM((NA, TB, 512), BF16), pltpu.VMEM((NA, 3, TB, 256), BF16),
                pltpu.VMEM((NB, TB, 256), BF16), pltpu.VMEM((NB, TB, 512), BF16),
                pltpu.VMEM(r_qkv.shape, F32), pltpu.VMEM(c_qkv.shape, F32),
                pltpu.VMEM(r_out.shape, F32), pltpu.VMEM(c_out.shape, F32),
                pltpu.VMEM((3, 512, 128), F32), pltpu.VMEM((256, 128), F32),
                pltpu.VMEM((12, 128, 128), F32), pltpu.VMEM((2, 4 * n_layers, 8, 128), F32),
                pltpu.VMEM((n_layers, ATT, 12, 128), F32), pltpu.VMEM((n_layers, EMB, 6, 128), F32),
                pltpu.VMEM((n_layers, ATT, 4, 128), F32), pltpu.VMEM((n_layers, EMB, 2, 128), F32),
                pltpu.VMEM((ATT * EMB, 1, 128), F32),
                pltpu.VMEM((n_layers, 12, 128), F32), pltpu.VMEM((n_layers, 6, 128), F32),
                pltpu.VMEM((n_layers, 2, 128), F32), pltpu.VMEM((n_layers, 4, 128), F32),
                pltpu.VMEM((1, 128), F32),
                pltpu.SemaphoreType.DMA((NA, 2 * TB // SUB)), pltpu.SemaphoreType.DMA((NB, 2 * TB // SUB)),
                pltpu.SemaphoreType.DMA((n_layers, 2)), pltpu.SemaphoreType.DMA((4,)),
                pltpu.SemaphoreType.DMA((4, n_layers)), pltpu.SemaphoreType.DMA((4, n_layers)),
                pltpu.SemaphoreType.DMA, pltpu.SemaphoreType.DMA,
            ],
            compiler_params=pltpu.CompilerParams(
                collective_id=0, has_side_effects=True, vmem_limit_bytes=45 * 2**20
            ),
            name="adafactor_step",
        )(hyper_params, x_in, dy_qkv, x_attn, dy_out, w_qkv, w_out, r_qkv, c_qkv, r_out, c_out)
        wn_qkv, wn_out, rn_qkv, cn_qkv, rn_out, cn_out = pl.pallas_call(
            functools.partial(write_kernel, n_layers),
            out_shape=(like(w_qkv), like(w_out), like(r_qkv), like(c_qkv), like(r_out), like(c_out)),
            in_specs=[vmem] * 9,
            out_specs=[hbm] * 6,
            scratch_shapes=[
                pltpu.VMEM(w_qkv.shape, F32), pltpu.VMEM(w_out.shape, F32),
                pltpu.VMEM(r_qkv.shape, F32), pltpu.VMEM(c_qkv.shape, F32),
                pltpu.VMEM(r_out.shape, F32), pltpu.VMEM(c_out.shape, F32),
                pltpu.SemaphoreType.DMA((4 * n_layers + 3,)), pltpu.SemaphoreType.DMA((4,)),
            ],
            compiler_params=pltpu.CompilerParams(vmem_limit_bytes=16 * 2**20),
            name="adafactor_write",
        )(*mids)
        return wn_qkv, wn_out, jnp.swapaxes(rn_qkv, 0, 1), jnp.swapaxes(cn_qkv, 0, 1), rn_out, cn_out

    return jax.shard_map(
        local_run,
        mesh=mesh,
        in_specs=(qkv, out, row, P(None, None, None, "att"), col, row, row, col, P(None, "att"), P(None, "emb"), P()),
        out_specs=(qkv, out, row, col, P(None, "att"), P(None, "emb")),
        check_vma=False,
    )
```

```python
import functools

import jax
import jax.numpy as jnp
from jax import lax
from jax.experimental import pallas as pl
from jax.experimental.pallas import tpu as pltpu
from jax.sharding import PartitionSpec as P

EPS_SQUARE = 1e-30
EPS_SCALE = 1e-3
F32 = jnp.float32
BF16 = jnp.bfloat16
MESH = pl.DeviceIdType.MESH
TB = 2048
SUB = 2048
NA = 3
NB = 3
ATT = 8
EMB = 4


def rows_to_lanes(part):
    return jnp.sum(part.T, axis=0, keepdims=True)


def fold8(part):
    return jnp.sum(part.reshape(part.shape[0] // 8, 8, 128), axis=0)


def total(part):
    return jnp.sum(jnp.sum(part, axis=0, keepdims=True), axis=1, keepdims=True)


def step_kernel(
    n_layers, n_tokens, d_model,
    hyper, x_in, dy_qkv, x_attn, dy_out, w_qkv, w_out, r_qkv, c_qkv, r_out, c_out,
    u_qkv, u_out, wv_qkv, wv_out, scales, rn_qkv, cn_qkv, rn_out, cn_out,
    xb, dyb, xab, dob, rq, cq, ro, co, row_a, row_b, a_cols, parts,
    att_a, emb_a, att_b, emb_b, glob, old_a, old_ac, old_b, old_bc, payload,
    sem_a, sem_b, sem_w, sem_s, send_sem, recv_sem, send_g, recv_g,
):
    nb = n_tokens // TB
    me_att = lax.axis_index("att")
    me_emb = lax.axis_index("emb")

    def copies_a(g, subs=range(TB // SUB)):
        l, i, s = g // nb, g % nb, g % NA
        copies = []
        for n in subs:
            src = pl.ds(pl.multiple_of(i * TB + n * SUB, SUB), SUB)
            dst = pl.ds(n * SUB, SUB)
            copies.append(pltpu.make_async_copy(x_in.at[l, src], xb.at[s, dst], sem_a.at[s, 2 * n]))
            copies.append(pltpu.make_async_copy(dy_qkv.at[l, :, src], dyb.at[s, :, dst], sem_a.at[s, 2 * n + 1]))
        return copies

    def copies_b(g, subs=range(TB // SUB)):
        l, i, s = g // nb, g % nb, g % NB
        copies = []
        for n in subs:
            src = pl.ds(pl.multiple_of(i * TB + n * SUB, SUB), SUB)
            dst = pl.ds(n * SUB, SUB)
            copies.append(pltpu.make_async_copy(x_attn.at[l, src], xab.at[s, dst], sem_b.at[s, 2 * n]))
            copies.append(pltpu.make_async_copy(dy_out.at[l, src], dob.at[s, dst], sem_b.at[s, 2 * n + 1]))
        return copies

    def copies_w(l):
        return (
            pltpu.make_async_copy(w_qkv.at[l], wv_qkv.at[l], sem_w.at[l, 0]),
            pltpu.make_async_copy(w_out.at[l], wv_out.at[l], sem_w.at[l, 1]),
        )

    def start(copies):
        for copy in copies:
            copy.start()

    def wait(copies):
        for copy in copies:
            copy.wait()

    def send_att(buf, kind, l):
        for d in (4, 3, 5, 2, 6, 1, 7):
            pltpu.make_async_remote_copy(
                src_ref=buf.at[l, 0], dst_ref=buf.at[l, ATT - d],
                send_sem=send_sem.at[kind, l], recv_sem=recv_sem.at[kind, l],
                device_id={"att": lax.rem(me_att + d, ATT)}, device_id_type=MESH,
            ).start()

    def send_emb(buf, kind, l):
        for d in (2, 1, 3):
            pltpu.make_async_remote_copy(
                src_ref=buf.at[l, 0], dst_ref=buf.at[l, EMB - d],
                send_sem=send_sem.at[kind, l], recv_sem=recv_sem.at[kind, l],
                device_id={"emb": lax.rem(me_emb + d, EMB)}, device_id_type=MESH,
            ).start()

    def wait_group(buf, n, kind, l):
        others = buf.at[l, pl.ds(1, n - 1)]
        pltpu.make_async_copy(others, others, send_sem.at[kind, l]).wait()
        pltpu.make_async_copy(others, others, recv_sem.at[kind, l]).wait()

    small = [
        pltpu.make_async_copy(src, dst, sem_s.at[n])
        for n, (src, dst) in enumerate(((r_qkv, rq), (c_qkv, cq), (r_out, ro), (c_out, co)))
    ]
    start(small)
    for n in range(TB // SUB):
        start(copies_a(jnp.int32(0), (n,)))
        start(copies_b(jnp.int32(0), (n,)))
    for g in range(1, NA):
        start(copies_a(jnp.int32(g)))
        start(copies_b(jnp.int32(g)))

    barrier = pltpu.get_barrier_semaphore()
    for da in range(ATT):
        for de in range(EMB):
            if da or de:
                pl.semaphore_signal(
                    barrier, inc=1,
                    device_id={"att": lax.rem(me_att + da, ATT), "emb": lax.rem(me_emb + de, EMB)},
                    device_id_type=MESH,
                )
    payload[...] = jnp.zeros_like(payload)

    beta = hyper[0]
    gain = 1.0 - beta

    def prepare():
        wait(small)
        for l in range(n_layers):
            for k in range(3):
                for j in range(4):
                    old_a[l, k * 4 + j : k * 4 + j + 1, :] = rq[k, l : l + 1, j * 128 : (j + 1) * 128]
                for j in range(2):
                    old_ac[l, k * 2 + j : k * 2 + j + 1, :] = cq[k, l : l + 1, j * 128 : (j + 1) * 128]
            for j in range(2):
                old_b[l, j : j + 1, :] = ro[l : l + 1, j * 128 : (j + 1) * 128]
            for j in range(4):
                old_bc[l, j : j + 1, :] = co[l : l + 1, j * 128 : (j + 1) * 128]
        pl.semaphore_wait(barrier, ATT * EMB - 1)

    def mul_a(l, s, keep, part=slice(None)):
        grads = jnp.concatenate([dyb[s, k, part] for k in range(3)], axis=1)
        prod = lax.dot_general(xb[s, part], grads, (((0,), (0,)), ((), ())), preferred_element_type=F32)
        for k in range(3):
            u_qkv[l, k] = jnp.where(keep, u_qkv[l, k], 0.0) + prod[:, k * 256 : (k + 1) * 256]

    def mul_b(l, s, keep, part=slice(None)):
        prod = lax.dot_general(xab[s, part], dob[s, part], (((0,), (0,)), ((), ())), preferred_element_type=F32)
        u_out[l] = jnp.where(keep, u_out[l], 0.0) + prod

    def refill_a(g):
        @pl.when(g + NA < n_layers * nb)
        def _():
            start(copies_a(g + NA))

    def refill_b(g):
        @pl.when(g + NB < n_layers * nb)
        def _():
            start(copies_b(g + NB))

    def stats_a(l):
        for k in range(3):
            cols = None
            for q in range(2):
                g = u_qkv[l, k, pl.ds(q * 256, 256)]
                sq = g * g
                row_a[k, pl.ds(q * 256, 256)] = sq[:, :128] + sq[:, 128:]
                part = jnp.sum(sq, axis=0, keepdims=True)
                cols = part if cols is None else cols + part
            for j in range(2):
                emb_a[l, 0, k * 2 + j : k * 2 + j + 1, :] = cols[:, j * 128 : (j + 1) * 128]
        for k in range(3):
            rows = rows_to_lanes(row_a[k])
            for j in range(4):
                att_a[l, 0, k * 4 + j : k * 4 + j + 1, :] = rows[:, j * 128 : (j + 1) * 128]
        send_att(att_a, 0, l)
        send_emb(emb_a, 1, l)

    def stats_b(l):
        parts = []
        for q in range(2):
            g = u_out[l, :, pl.ds(q * 256, 256)]
            sq = g * g
            parts.append(sq[:, :128] + sq[:, 128:])
            cols = jnp.sum(sq, axis=0, keepdims=True)
            for j in range(2):
                att_b[l, 0, q * 2 + j : q * 2 + j + 1, :] = cols[:, j * 128 : (j + 1) * 128]
            if q == 0:
                row_b[...] = parts[0]
            else:
                row_b[...] = row_b[...] + parts[1]
        rows = rows_to_lanes(row_b[...])
        for j in range(2):
            emb_b[l, 0, j : j + 1, :] = rows[:, j * 128 : (j + 1) * 128]
        send_att(att_b, 2, l)
        send_emb(emb_b, 3, l)

    def record(slot, value):
        lane = lax.broadcasted_iota(jnp.int32, (1, 128), 1)
        payload[...] = jnp.where(lane == 8 * slot, value, payload[...])

    def sum_w(l):
        wait(copies_w(l))
        for k in range(3):
            w = wv_qkv[l, k]
            parts[1, l * 4 + k] = fold8(w[:, :128] * w[:, :128] + w[:, 128:] * w[:, 128:])
        w = wv_out[l]
        parts[1, l * 4 + 3] = sum(fold8(w[:, j * 128 : (j + 1) * 128] * w[:, j * 128 : (j + 1) * 128]) for j in range(4))

    def apply_a(l):
        row_sum = att_a[l, 0]
        for d in range(1, ATT):
            row_sum = row_sum + att_a[l, d]
        col_sum = emb_a[l, 0]
        for d in range(1, EMB):
            col_sum = col_sum + emb_a[l, d]
        r_new = beta * old_a[l] + gain * (row_sum * (1.0 / d_model) + EPS_SQUARE)
        c_new = beta * old_ac[l] + gain * (col_sum * (1.0 / d_model) + EPS_SQUARE)
        rn_qkv[l] = r_new
        cn_qkv[l] = c_new
        b_all = lax.rsqrt(c_new)
        means = [total(r_new[k * 4 : (k + 1) * 4]) * (1.0 / 512) for k in range(3)]
        for k in range(3):
            a_k = lax.rsqrt(r_new[k * 4 : (k + 1) * 4] / means[k])
            for j in range(4):
                a_cols[k * 4 + j] = jnp.broadcast_to(a_k[j : j + 1], (128, 128)).T
        for k in range(3):
            tsum = jnp.zeros((8, 128), F32)
            for j in range(4):
                a_col = a_cols[k * 4 + j]
                for h in range(2):
                    rr, cc = pl.ds(j * 128, 128), pl.ds(h * 128, 128)
                    u = u_qkv[l, k, rr, cc] * a_col * b_all[k * 2 + h : k * 2 + h + 1]
                    u_qkv[l, k, rr, cc] = u
                    tsum = tsum + fold8(u * u)
            parts[0, l * 4 + k] = tsum
            record(l * 4 + k, means[k])

    def apply_b(l):
        col_sum = att_b[l, 0]
        for d in range(1, ATT):
            col_sum = col_sum + att_b[l, d]
        row_sum = emb_b[l, 0]
        for d in range(1, EMB):
            row_sum = row_sum + emb_b[l, d]
        r_new = beta * old_b[l] + gain * (row_sum * (1.0 / d_model) + EPS_SQUARE)
        c_new = beta * old_bc[l] + gain * (col_sum * (1.0 / d_model) + EPS_SQUARE)
        b_all = lax.rsqrt(c_new)
        mean = total(r_new) * (1.0 / 256)
        a_all = lax.rsqrt(r_new / mean)
        tsum = jnp.zeros((8, 128), F32)
        for j in range(2):
            a_col = jnp.broadcast_to(a_all[j : j + 1], (128, 128)).T
            for h in range(4):
                rr, cc = pl.ds(j * 128, 128), pl.ds(h * 128, 128)
                u = u_out[l, rr, cc] * a_col * b_all[h : h + 1]
                u_out[l, rr, cc] = u
                tsum = tsum + fold8(u * u)
        rn_out[l] = r_new
        cn_out[l] = c_new
        parts[0, l * 4 + 3] = tsum
        record(l * 4 + 3, mean)

    last = n_layers - 1

    def per_matrix(n):
        sums = rows_to_lanes(parts[n].reshape(128, 128))
        for shift in (4, 2, 1):
            sums = sums + pltpu.roll(sums, 128 - shift, 1)
        return sums

    def arrive_a(l):
        wait_group(att_a, ATT, 0, l)
        wait_group(emb_a, EMB, 1, l)

    def arrive_b(l):
        wait_group(att_b, ATT, 2, l)
        wait_group(emb_b, EMB, 3, l)

    def piece(n, carry):
        part = pl.ds(pl.multiple_of(n * SUB, SUB), SUB)
        for m in range(TB // SUB):
            @pl.when(n == m)
            def _():
                wait(copies_a(jnp.int32(0), (m,)))
                wait(copies_b(jnp.int32(0), (m,)))

        mul_a(0, 0, n > 0, part)
        mul_b(0, 0, n > 0, part)
        return carry

    lax.fori_loop(0, TB // SUB, piece, 0)
    refill_a(jnp.int32(0))
    refill_b(jnp.int32(0))

    def layer(l, carry):
        def block(i, carry):
            g = l * nb + i
            wait(copies_a(g))
            wait(copies_b(g))
            mul_a(l, g % NA, i > 0)
            mul_b(l, g % NB, i > 0)
            refill_a(g)
            refill_b(g)
            return carry

        lax.fori_loop(jnp.where(l == 0, 1, 0), nb, block, 0)

        @pl.when(l == 0)
        def _():
            prepare()

        stats_a(l)
        stats_b(l)
        return carry

    lax.fori_loop(0, last, layer, 0)

    def block_a(i, carry):
        g = last * nb + i
        wait(copies_a(g))
        mul_a(last, g % NA, i > 0)
        return carry

    lax.fori_loop(0, nb, block_a, 0)
    for l in range(n_layers):
        start(copies_w(l))
    stats_a(last)

    for n in range(nb):
        wait(copies_b(jnp.int32(last * nb + n)))
    lhs, rhs = xab[...].reshape(n_tokens, 256), dob[...].reshape(n_tokens, 512)
    u_out[last] = lax.dot_general(lhs, rhs, (((0,), (0,)), ((), ())), preferred_element_type=F32)
    stats_b(last)

    def earlier(l, carry):
        arrive_a(l)
        arrive_b(l)
        apply_a(l)
        apply_b(l)
        return carry

    lax.fori_loop(0, last, earlier, 0)

    def weights(l, carry):
        sum_w(l)
        return carry

    lax.fori_loop(0, n_layers, weights, 0)
    arrive_a(last)
    apply_a(last)
    w_parts = per_matrix(1)
    arrive_b(last)
    apply_b(last)

    phase = lax.broadcasted_iota(jnp.int32, (1, 128), 1) & 7
    row = jnp.where(phase == 1, pltpu.roll(w_parts, 1, 1), pltpu.roll(payload[...], 2, 1))
    glob[0] = jnp.where(phase == 0, per_matrix(0) / payload[...], row)
    for da in (4, 3, 5, 2, 6, 1, 7, 0):
        for de in (2, 3, 1, 0):
            if da or de:
                pltpu.make_async_remote_copy(
                    src_ref=glob.at[0], dst_ref=glob.at[((ATT - da) % ATT) * EMB + (EMB - de) % EMB],
                    send_sem=send_g, recv_sem=recv_g,
                    device_id={"att": lax.rem(me_att + da, ATT), "emb": lax.rem(me_emb + de, EMB)},
                    device_id_type=MESH,
                ).start()
    others = glob.at[pl.ds(1, ATT * EMB - 1)]
    pltpu.make_async_copy(others, others, send_g).wait()
    pltpu.make_async_copy(others, others, recv_g).wait()
    n_dev = ATT * EMB
    sums = glob[0]
    for d in range(1, n_dev):
        sums = sums + glob[d]
    mean_all = pltpu.roll(sums, 128 - 2, 1) * (1.0 / n_dev)
    w_sum = pltpu.roll(sums, 128 - 1, 1)
    u_sum = sums * mean_all
    n_elems = float(d_model) * d_model
    rms_u = jnp.sqrt(u_sum * (1.0 / n_elems))
    rms_w = jnp.sqrt(w_sum * (1.0 / n_elems))
    step = hyper[1] * jnp.maximum(EPS_SCALE, rms_w) / jnp.maximum(1.0, rms_u / hyper[2])
    scales[...] = step * jnp.sqrt(mean_all / payload[...])


def write_kernel(
    n_layers, u_qkv, u_out, wv_qkv, wv_out, scales, rn_qkv, cn_qkv, rn_out, cn_out,
    wn_qkv, wn_out, r_qkv, c_qkv, r_out, c_out,
    st_a, st_b, st_rq, st_cq, st_r, st_c, sem_w, sem_s,
):
    copies = []
    for l in range(n_layers):
        for k in range(4):
            m = l * 4 + k
            s = scales[0:1, 8 * m : 8 * m + 1]
            parts = 4 if m == 0 else 1
            for n in range(parts):
                if k < 3:
                    rows = pl.ds(n * (512 // parts), 512 // parts)
                    st_a[l, k, rows] = wv_qkv[l, k, rows] - s * u_qkv[l, k, rows]
                    copy = pltpu.make_async_copy(st_a.at[l, k, rows], wn_qkv.at[l, k, rows], sem_w.at[m if n == 0 else 15 + n])
                else:
                    st_b[l] = wv_out[l] - s * u_out[l]
                    copy = pltpu.make_async_copy(st_b.at[l], wn_out.at[l], sem_w.at[m])
                copy.start()
                copies.append(copy)
    for l in range(n_layers):
        for k in range(3):
            for j in range(4):
                st_rq[k, l : l + 1, j * 128 : (j + 1) * 128] = rn_qkv[l, k * 4 + j : k * 4 + j + 1]
            for j in range(2):
                st_cq[k, l : l + 1, j * 128 : (j + 1) * 128] = cn_qkv[l, k * 2 + j : k * 2 + j + 1]
        for j in range(2):
            st_r[l : l + 1, j * 128 : (j + 1) * 128] = rn_out[l, j : j + 1]
        for j in range(4):
            st_c[l : l + 1, j * 128 : (j + 1) * 128] = cn_out[l, j : j + 1]
    small = [
        pltpu.make_async_copy(src, dst, sem_s.at[n])
        for n, (src, dst) in enumerate(((st_rq, r_qkv), (st_cq, c_qkv), (st_r, r_out), (st_c, c_out)))
    ]
    for copy in small:
        copy.start()
    for copy in copies + small:
        copy.wait()


def solution(mesh):
    att, emb = mesh.shape["att"], mesh.shape["emb"]
    qkv = P(None, None, "emb", "att")
    out = P(None, "att", "emb")
    row = P(None, None, "emb")
    col = P(None, None, "att")

    def local_run(w_qkv, w_out, x_in, dy_qkv, x_attn, dy_out, r_qkv, c_qkv, r_out, c_out, hyper_params):
        n_layers, n_tokens = x_in.shape[:2]
        d_model = x_in.shape[2] * emb
        hbm = pl.BlockSpec(memory_space=pltpu.HBM)
        vmem = pl.BlockSpec(memory_space=pltpu.VMEM)
        smem = pl.BlockSpec(memory_space=pltpu.SMEM)
        like = lambda x: jax.ShapeDtypeStruct(x.shape, x.dtype)
        kept = lambda x: pltpu.VMEM(x.shape, x.dtype)
        stat = lambda n: pltpu.VMEM((n_layers, n, 128), F32)
        r_qkv, c_qkv = jnp.swapaxes(r_qkv, 0, 1), jnp.swapaxes(c_qkv, 0, 1)
        mids = pl.pallas_call(
            functools.partial(step_kernel, n_layers, n_tokens, d_model),
            out_shape=(
                kept(w_qkv), kept(w_out), kept(w_qkv), kept(w_out), pltpu.VMEM((1, 128), F32),
                stat(12), stat(6), stat(2), stat(4),
            ),
            in_specs=[smem] + [hbm] * 10,
            out_specs=[vmem] * 9,
            scratch_shapes=[
                pltpu.VMEM((NA, TB, 512), BF16), pltpu.VMEM((NA, 3, TB, 256), BF16),
                pltpu.VMEM((NB, TB, 256), BF16), pltpu.VMEM((NB, TB, 512), BF16),
                pltpu.VMEM(r_qkv.shape, F32), pltpu.VMEM(c_qkv.shape, F32),
                pltpu.VMEM(r_out.shape, F32), pltpu.VMEM(c_out.shape, F32),
                pltpu.VMEM((3, 512, 128), F32), pltpu.VMEM((256, 128), F32),
                pltpu.VMEM((12, 128, 128), F32), pltpu.VMEM((2, 4 * n_layers, 8, 128), F32),
                pltpu.VMEM((n_layers, ATT, 12, 128), F32), pltpu.VMEM((n_layers, EMB, 6, 128), F32),
                pltpu.VMEM((n_layers, ATT, 4, 128), F32), pltpu.VMEM((n_layers, EMB, 2, 128), F32),
                pltpu.VMEM((ATT * EMB, 1, 128), F32),
                pltpu.VMEM((n_layers, 12, 128), F32), pltpu.VMEM((n_layers, 6, 128), F32),
                pltpu.VMEM((n_layers, 2, 128), F32), pltpu.VMEM((n_layers, 4, 128), F32),
                pltpu.VMEM((1, 128), F32),
                pltpu.SemaphoreType.DMA((NA, 2 * TB // SUB)), pltpu.SemaphoreType.DMA((NB, 2 * TB // SUB)),
                pltpu.SemaphoreType.DMA((n_layers, 2)), pltpu.SemaphoreType.DMA((4,)),
                pltpu.SemaphoreType.DMA((4, n_layers)), pltpu.SemaphoreType.DMA((4, n_layers)),
                pltpu.SemaphoreType.DMA, pltpu.SemaphoreType.DMA,
            ],
            compiler_params=pltpu.CompilerParams(
                collective_id=0, has_side_effects=True, vmem_limit_bytes=45 * 2**20
            ),
            name="adafactor_step",
        )(hyper_params, x_in, dy_qkv, x_attn, dy_out, w_qkv, w_out, r_qkv, c_qkv, r_out, c_out)
        wn_qkv, wn_out, rn_qkv, cn_qkv, rn_out, cn_out = pl.pallas_call(
            functools.partial(write_kernel, n_layers),
            out_shape=(like(w_qkv), like(w_out), like(r_qkv), like(c_qkv), like(r_out), like(c_out)),
            in_specs=[vmem] * 9,
            out_specs=[hbm] * 6,
            scratch_shapes=[
                pltpu.VMEM(w_qkv.shape, F32), pltpu.VMEM(w_out.shape, F32),
                pltpu.VMEM(r_qkv.shape, F32), pltpu.VMEM(c_qkv.shape, F32),
                pltpu.VMEM(r_out.shape, F32), pltpu.VMEM(c_out.shape, F32),
                pltpu.SemaphoreType.DMA((4 * n_layers + 3,)), pltpu.SemaphoreType.DMA((4,)),
            ],
            compiler_params=pltpu.CompilerParams(vmem_limit_bytes=16 * 2**20),
            name="adafactor_write",
        )(*mids)
        return wn_qkv, wn_out, jnp.swapaxes(rn_qkv, 0, 1), jnp.swapaxes(cn_qkv, 0, 1), rn_out, cn_out

    return jax.shard_map(
        local_run,
        mesh=mesh,
        in_specs=(qkv, out, row, P(None, None, None, "att"), col, row, row, col, P(None, "att"), P(None, "emb"), P()),
        out_specs=(qkv, out, row, col, P(None, "att"), P(None, "emb")),
        check_vma=False,
    )
```
